256 devices in a mesh: section: 4 (over y), owner: 64 (over x, z, core).
Axes of the slice: x: 4, y: 4, z: 8, core: 2. Of those that a mesh axis runs over, the one named last changes fastest.
Arguments:
- weights: bfloat16 [4, 1024, 1024], P('section'), may hold values from -0.1875 to 0.1875
- inputs: bfloat16 [4, 4, 16384, 1024], P('section', None, 'owner'), may hold values from -16 to 16
- preact: bfloat16 [4, 4, 16384, 1024], P('section', None, 'owner'), may hold values from -6 to 6
- cotangent: bfloat16 [4, 16384, 1024], P(None, 'owner'), may hold values from -6 to 6
- embeddings: bfloat16 [4, 16384, 32, 128], P(None, ('owner', 'section')), may hold values from -6 to 6
- row_ids: int32 [4, 16384, 32], P(None, ('owner', 'section')), may hold values from 0 to 1023
Outputs:
- weight_grad: float32 [4, 1024, 1024], P('section', 'owner')
- table_grad: float32 [64, 512, 128], P('owner', 'section')
The draws below stay inside these ranges and needn't reach their ends.
All inputs are finite; a program needn't handle non-finite values.
Results may differ from the reference program's by a relative error of at most 0.0064.
Values may be sent and summed in bfloat16 or wider, within the bound.
A program may use at most 128 MiB of HBM per device.

```python
import math
import jax
import jax.numpy as jnp
import numpy as np
from jax import lax

F = 32
E = 128
H = 1024
MICRO = 4
TROWS = 512
LAYERS = 4
SLOTS = 64
ROWS = 1024
BATCH = 16384


def with_ends(values, own_key, low, high):
    longest = values.shape.index(max(values.shape))
    spots = []
    for shift in (0, 1):
        where = [jax.random.randint(jax.random.fold_in(own_key, axis), (), 0, length) for axis, length in enumerate(values.shape)]
        where[longest] = (where[longest] + shift) % values.shape[longest]
        spots.append(tuple(where))
    return values.at[spots[0]].set(low).at[spots[1]].set(high)


def spiked(drawn, key, source, target, blocks, factor):
    def block_of(dim):
        return (jnp.arange(drawn.shape[dim]) // (drawn.shape[dim] // blocks)).reshape((-1,) + (1,) * (drawn.ndim - 1 - dim))

    near = jax.random.permutation(key, blocks)[block_of(target)]
    other_side = (block_of(target) + blocks // 2) % blocks
    return jnp.where((block_of(source) == near) | (block_of(source) == other_side), factor * drawn, drawn)


def shard_levels(key, extent, split, least, top_value):
    loudness = 1.0
    for dim, shards_of in split:
        draws = jax.random.uniform(jax.random.fold_in(jax.random.fold_in(key, 6), dim), (shards_of,), jnp.float32, least / len(split), top_value / len(split))
        loudness = loudness * jnp.repeat(jnp.exp(draws), extent[dim] // shards_of).reshape((-1,) + (1,) * (len(extent) - 1 - dim))
    return loudness


def rank_bounds(amount, skew):
    weights = [(1 << 20) // math.isqrt(standing ** skew) + 1 for standing in range(1, amount + 1)]
    deviation = 1 + sum(weights) // (1 << 30)
    return np.cumsum(np.array([max(1, weight // deviation) for weight in weights]))


def skewed_ids(stream_key, dims, number_of, skew):
    listing = rank_bounds(number_of, skew)
    ticket = jax.random.randint(jax.random.fold_in(stream_key, 1), dims, 0, int(listing[number_of - 1]))
    grade = jnp.searchsorted(jnp.asarray(listing, jnp.int32), ticket, side="right")
    return jax.random.permutation(jax.random.fold_in(stream_key, 2), number_of)[grade].astype(jnp.int32)


def gaussian(key, extent, width, limit, pieces=(), held_as=jnp.bfloat16):
    drawn = width * jax.random.normal(key, extent, jnp.float32)
    if pieces:
        drawn = drawn * shard_levels(key, extent, pieces, -0.22, 0.18)
    return jnp.clip(drawn, -limit, limit).astype(held_as)


def gaussian_with(rng, extent, spread, limit, pieces, heavy, kind=jnp.bfloat16):
    values = spread * jax.random.normal(rng, extent, jnp.float32)
    if pieces:
        values = values * shard_levels(rng, extent, pieces, -0.22, 0.18)
    return jnp.clip(spiked(values, jax.random.fold_in(rng, 3), *heavy), -limit, limit).astype(kind)


def setup_inputs(seed: int = 0) -> dict:
    arg_keys = jax.random.split(jax.random.key(seed), 7)
    return {
        "weights": gaussian(arg_keys[0], (LAYERS, H, H), H ** -0.5, 0.1875, ((0, 4),)),
        "inputs": gaussian_with(arg_keys[1], (LAYERS, MICRO, BATCH, H), 1.0, 16.0, ((0, 4), (2, 64)), (2, 3, 64, 4.0)),
        "preact": gaussian(arg_keys[2], (LAYERS, MICRO, BATCH, H), 1.0, 6.0, ((0, 4), (2, 64))),
        "cotangent": gaussian(arg_keys[3], (MICRO, BATCH, H), 1.0, 6.0, ((1, 64),)),
        "embeddings": gaussian(arg_keys[4], (MICRO, BATCH, F, E), 1.0, 6.0, ((1, 256),)),
        "row_ids": with_ends(skewed_ids(arg_keys[5], (MICRO, BATCH, F), ROWS, 2), jax.random.fold_in(arg_keys[5], 3), 0, ROWS - 1).astype(jnp.int32),
    }


def reference(weights, inputs, preact, cotangent, embeddings, row_ids):
    highest = lax.Precision.HIGHEST
    micro_count, sample_rows, hidden = cotangent.shape
    features = embeddings.shape[2]
    emb_width = embeddings.shape[3]
    grad_scale = 1.0 / math.sqrt(micro_count * sample_rows)
    upstream = cotangent
    layer_grads = []
    for layer_index in range(LAYERS - 1, -1, -1):
        slope = jnp.where(preact[layer_index] > 0, upstream, jnp.zeros_like(upstream))
        slope = slope.reshape(micro_count * sample_rows, hidden)
        flat_in = inputs[layer_index].reshape(micro_count * sample_rows, hidden)
        layer_grads.append(jnp.dot(flat_in.T.astype(jnp.float32), slope.astype(jnp.float32), precision=highest) * grad_scale)
        upstream = jnp.dot(slope.astype(jnp.float32), weights[layer_index].T.astype(jnp.float32), precision=highest)
        upstream = upstream.astype(jnp.bfloat16).reshape(micro_count, sample_rows, hidden)
    weight_grad = jnp.stack(layer_grads[::-1])

    def feature_grads(members):
        flat_grad, embedded = members
        square = flat_grad.reshape(sample_rows, features, features).astype(jnp.float32)
        emb32 = embedded.astype(jnp.float32)
        direct = jnp.einsum('qfg,qge->qfe', square, emb32, precision=highest)
        swapped = jnp.einsum('qgf,qge->qfe', square, emb32, precision=highest)
        return (direct + swapped).astype(jnp.bfloat16)
    grads_all = lax.map(feature_grads, (upstream, embeddings))
    flat_grads = grads_all.reshape(micro_count * sample_rows, features, emb_width)
    flat_ids = row_ids.reshape(micro_count * sample_rows, features)

    def one_table(feature_index):
        column = lax.dynamic_index_in_dim(flat_grads, feature_index, 1, False).astype(jnp.float32)
        row_index = lax.dynamic_index_in_dim(flat_ids, feature_index, 1, False)
        return jax.ops.segment_sum(column, row_index, num_segments=ROWS)
    tables = lax.map(one_table, jnp.arange(features, dtype=jnp.int32))
    table_grad = (tables * grad_scale).reshape(SLOTS, TROWS, emb_width)
    return (weight_grad, table_grad)
```

```python
import math

import functools

import jax
import jax.numpy as jnp
from jax import lax
from jax.experimental import pallas as pl
from jax.experimental.pallas import tpu as pltpu
from jax.sharding import Mesh
from jax.sharding import PartitionSpec as P

TROWS = 512
OWNER = ("owner_0", "owner_1", "owner_2")
OWNER_SECTION = ("owner_0", "owner_1", "owner_2", "section")


def partner(block, axis, apart):
    count = lax.axis_size(axis)
    route = []
    for low in range(count):
        high = low | 1 << apart
        if high != low and high < count:
            route += [(low, high), (high, low)]
    return lax.ppermute(block, axis, route)


def passed_along(x, axis, by):
    count = lax.axis_size(axis)
    pairs = [(i, i + by) for i in range(count) if 0 <= i + by < count]
    return lax.ppermute(x, axis, pairs)


def cut_along(x, dim, count):
    lengths = x.shape
    parts = x.reshape(*lengths[:dim], count, lengths[dim] // count, *lengths[dim + 1 :])
    return jnp.moveaxis(parts, dim, 0)


def sum_at_owner(x, axis, dim):
    count = lax.axis_size(axis)
    parts = lax.all_to_all(cut_along(x, dim, count), axis, 0, 0, tiled=True)
    return jnp.sum(parts.astype(jnp.float32), axis=0)


def summed_on_arrival(x, axis, dim):
    count = lax.axis_size(axis)
    parts = lax.all_to_all(cut_along(x, dim, count), axis, 0, 0, tiled=True)
    return jnp.sum(parts, axis=0)


def sum_in_order(parts, axes, sequence):
    lengths = [lax.axis_size(a) for a in axes]
    parts = parts.reshape(*lengths, *parts.shape[1:])
    parts = parts.transpose(*sequence, *range(len(axes), parts.ndim))
    parts = parts.reshape(-1, *parts.shape[len(axes) :])
    for k in sequence:
        parts = lax.psum_scatter(parts, axes[k], scatter_dimension=0, tiled=True)
    return parts[0]


def sum_by_axis(x, axes, sequence, dim):
    count = lax.axis_size(axes)
    return sum_in_order(cut_along(x, dim, count), axes, sequence)


def pair_grads(flat_grad, embedded, features):
    sample_count = flat_grad.shape[0]
    square = flat_grad.reshape(sample_count, features, features)
    direct = jnp.einsum("qfg,qge->qfe", square, embedded, preferred_element_type=jnp.float32)
    swapped = jnp.einsum("qgf,qge->qfe", square, embedded, preferred_element_type=jnp.float32)
    return (direct + swapped).astype(jnp.bfloat16)


def spread_slots(feat_grads, feat_ids, row_split):
    sample_count, features, emb_width = feat_grads.shape
    portion_rows = sample_count // row_split
    grads_split = feat_grads.reshape(row_split, portion_rows, features, emb_width)
    grads_split = jnp.transpose(grads_split, (1, 2, 0, 3)).reshape(
        portion_rows, features * row_split, emb_width
    )
    ids_split = feat_ids.reshape(row_split, portion_rows, features)
    ids_split = jnp.transpose(ids_split, (1, 2, 0)).reshape(portion_rows, features * row_split)
    return (grads_split, ids_split)


def scatter_rows(arrived, local_row, row_total):
    sample_count, slot_count, emb_width = arrived.shape
    block_rows = math.gcd(sample_count, 2048)
    turns = sample_count // block_rows
    pieces_all = arrived.reshape(turns, block_rows, slot_count, emb_width)
    places_all = local_row.reshape(turns, block_rows, slot_count)
    positions = jnp.arange(row_total, dtype=jnp.int32)

    def add_block(running, members):
        pieces, places = members
        onehot = (places[..., None] == positions).astype(jnp.bfloat16)
        return (
            running
            + jnp.einsum("qsr,qse->sre", onehot, pieces, preferred_element_type=jnp.float32),
            None,
        )

    start_table = jnp.zeros((slot_count, row_total, emb_width), jnp.float32)
    running, unused = lax.scan(add_block, start_table, (pieces_all, places_all))
    return running


def table_rows(arrived, arrived_ids, row_split):
    return scatter_rows(arrived, arrived_ids, TROWS * row_split)


def settle_rows(partial_value, owner_pos):
    half_rows = partial_value.shape[1] // 2
    lower = partial_value[:, :half_rows]
    upper = partial_value[:, half_rows:]
    upper_side = owner_pos // 2**0 % 2 == 1
    kept = jnp.where(upper_side, upper, lower)
    sending = jnp.where(upper_side, lower, upper)
    partial_value = kept + partner(sending, OWNER, 0)
    return partial_value


def chain_kernel(
    micros, sections,
    w_hbm, pre_hbm, cot_hbm, slopes_out, p_out,
    w_v, pre_v, rbuf, sbuf,
    w_sem, pre_sem, in_sem, out_sem, p_recv, p_send,
):
    section = lax.axis_index("section")
    chunks = micros * sections
    rows = pre_v.shape[0] // chunks
    last = section == sections - 1

    def part(ref, t):
        return ref.at[pl.ds(pl.multiple_of(t * rows, rows), rows)]

    def pre_copy(t):
        return pltpu.make_async_copy(part(pre_hbm, t), part(pre_v, t), pre_sem.at[t])

    def cot_copy(t):
        return pltpu.make_async_copy(part(cot_hbm, t), part(rbuf, t), in_sem.at[t])

    def down_copy(t):
        return pltpu.make_async_remote_copy(
            src_ref=part(sbuf, t), dst_ref=part(rbuf, t),
            send_sem=out_sem.at[t], recv_sem=in_sem.at[t],
            device_id={"section": lax.rem(section + sections - 1, sections)},
            device_id_type=pl.DeviceIdType.MESH,
        )

    def p_copy(t):
        m = t // sections
        return pltpu.make_async_remote_copy(
            src_ref=part(sbuf, t), dst_ref=part(p_out, m),
            send_sem=p_send.at[t], recv_sem=p_recv.at[m],
            device_id={"section": lax.rem(t, sections)},
            device_id_type=pl.DeviceIdType.MESH,
        )

    w_copy = pltpu.make_async_copy(w_hbm, w_v, w_sem)
    w_copy.start()

    def begin(t, carry):
        pre_copy(t).start()

        @pl.when(last)
        def _():
            cot_copy(t).start()
        return carry

    lax.fori_loop(0, chunks, begin, 0)
    barrier = pltpu.get_barrier_semaphore()
    for d in range(1, sections):
        pl.semaphore_signal(
            barrier, inc=1, device_id={"section": lax.rem(section + d, sections)},
            device_id_type=pl.DeviceIdType.MESH,
        )
    pl.semaphore_wait(barrier, sections - 1)
    w_copy.wait()

    def step(t, carry):
        pre_copy(t).wait()

        @pl.when(last)
        def _():
            cot_copy(t).wait()

        @pl.when(jnp.logical_not(last))
        def _():
            down_copy(t).wait_recv()

        at = pl.ds(pl.multiple_of(t * rows, rows), rows)
        incoming = rbuf[at, :]
        slope = jnp.where(pre_v[at, :] > 0, incoming, jnp.zeros_like(incoming))
        slopes_out[at, :] = slope
        sbuf[at, :] = lax.dot_general(
            slope, w_v[...], (((1,), (1,)), ((), ())), preferred_element_type=jnp.float32
        ).astype(jnp.bfloat16)

        @pl.when(section > 0)
        def _():
            down_copy(t).start()

        @pl.when((section == 0) & (lax.rem(t, sections) > 0))
        def _():
            p_copy(t).start()

        @pl.when((section == 0) & (lax.rem(t, sections) == 0))
        def _():
            own = pl.multiple_of((t // sections) * rows, rows)
            p_out[pl.ds(own, rows), :] = sbuf[at, :]
        return carry

    lax.fori_loop(0, chunks, step, 0)

    def finish(t, carry):
        @pl.when(section > 0)
        def _():
            down_copy(t).wait_send()

        @pl.when((section == 0) & (lax.rem(t, sections) > 0))
        def _():
            p_copy(t).wait_send()
        return carry

    lax.fori_loop(0, chunks, finish, 0)

    @pl.when(section > 0)
    def _():
        def take(m, carry):
            p_copy(m * sections).wait_recv()
            return carry

        lax.fori_loop(0, micros, take, 0)


def chain(w, pre, cot, micros, sections):
    total, hidden = pre.shape
    chunks = micros * sections
    dma = pltpu.SemaphoreType.DMA
    vmem = pl.BlockSpec(memory_space=pltpu.VMEM)
    hbm = pl.BlockSpec(memory_space=pl.ANY)
    slopes, portion = pl.pallas_call(
        functools.partial(chain_kernel, micros, sections),
        out_shape=(
            jax.ShapeDtypeStruct((total, hidden), jnp.bfloat16),
            jax.ShapeDtypeStruct((total // sections, hidden), jnp.bfloat16),
        ),
        in_specs=[hbm] * 3,
        out_specs=(vmem, vmem),
        scratch_shapes=[
            pltpu.VMEM((hidden, hidden), jnp.bfloat16),
            pltpu.VMEM((total, hidden), jnp.bfloat16),
            pltpu.VMEM((total, hidden), jnp.bfloat16),
            pltpu.VMEM((total, hidden), jnp.bfloat16),
            dma, dma((chunks,)), dma((chunks,)), dma((chunks,)), dma((micros,)), dma((chunks,)),
        ],
        compiler_params=pltpu.CompilerParams(collective_id=0, has_side_effects=True,
                                             vmem_limit_bytes=32 * 1024 * 1024),
    )(w, pre, cot)
    return slopes, portion.reshape(micros, total // sections // micros, hidden)


def per_device(weights, inputs, preact, cotangent, embeddings, row_ids):
    sections = lax.axis_size("section")
    owners = lax.axis_size(OWNER)
    section_pos = lax.axis_index("section")
    owner_pos = lax.axis_index(OWNER)
    micro_count, batch_rows, hidden = cotangent.shape
    features = embeddings.shape[2]
    emb_width = embeddings.shape[3]
    row_split = max(1, owners // features)
    grad_scale = 1.0 / math.sqrt(micro_count * batch_rows * owners)
    layer_in = inputs[0]
    slopes, portion = chain(
        weights[0],
        preact.reshape(micro_count * batch_rows, hidden),
        cotangent.reshape(micro_count * batch_rows, hidden),
        micro_count,
        sections,
    )
    quarter = portion.shape[1]
    feat_grads = pair_grads(
        portion.reshape(micro_count * quarter, hidden),
        embeddings.reshape(micro_count * quarter, features, emb_width),
        features,
    )
    outgoing, out_ids = spread_slots(
        feat_grads, row_ids.reshape(micro_count * quarter, features), row_split
    )
    arrived = lax.all_to_all(outgoing, OWNER, split_axis=1, concat_axis=0, tiled=True)
    arrived_ids = lax.all_to_all(out_ids, OWNER, split_axis=1, concat_axis=0, tiled=True)
    row_table = table_rows(arrived, arrived_ids, row_split)
    row_table = settle_rows(row_table, owner_pos)
    table_grad = summed_on_arrival(row_table, "section", 1) * grad_scale
    flat_in = layer_in.reshape(micro_count * batch_rows, hidden)
    flat_slope = slopes.reshape(micro_count * batch_rows, hidden)
    weight_grad = (
        sum_by_axis(
            lax.dot_general(
                flat_in, flat_slope, (((0,), (0,)), ((), ())), preferred_element_type=jnp.float32
            ),
            OWNER,
            (2, 0, 1),
            0,
        )
        * grad_scale
    )
    return (weight_grad[None], table_grad)


def solution(mesh):
    finer = Mesh(
        mesh.devices.reshape(mesh.shape["section"], 4, 8, 2),
        ("section", "owner_0", "owner_1", "owner_2"),
    )
    placed = (
        P("section", None, None),
        P("section", None, OWNER, None),
        P("section", None, OWNER, None),
        P(None, OWNER, None),
        P(None, OWNER_SECTION, None, None),
        P(None, OWNER_SECTION, None),
    )
    return jax.shard_map(
        per_device,
        mesh=finer,
        in_specs=placed,
        out_specs=(P("section", OWNER, None), P(OWNER, "section", None)),
        check_vma=False,
    )
```

```python
import functools
import math

import jax
import jax.numpy as jnp
from jax import lax
from jax.experimental import pallas as pl
from jax.experimental.pallas import tpu as pltpu
from jax.sharding import Mesh
from jax.sharding import PartitionSpec as P

OWNER = ("owner_0", "owner_1", "owner_2")
OWNER_SECTION = ("owner_0", "owner_1", "owner_2", "section")
MESH = pl.DeviceIdType.MESH
BF16 = jnp.bfloat16
F32 = jnp.float32
NN = (((1,), (0,)), ((), ()))
NT = (((1,), (1,)), ((), ()))
TN = (((0,), (0,)), ((), ()))
GROUP = 16


def dot(a, b, dims):
    return lax.dot_general(a, b, dims, preferred_element_type=F32)


def step_kernel(
    dims, scale,
    w_hbm, x_hbm, pre_hbm, cot_hbm, emb_hbm, ids_hbm,
    wg_out, tg_out,
    w_v, x_v, pre_v, emb_v, ids_v, rbuf, sbuf, slopes, pbuf, wacc, wrecv, wx, wxr, wz, wzr,
    fold, pick, spread, fg, arr, idr, onehot, acc, sib, yrecv,
    w_sem, x_sem, pre_sem, emb_sem, ids_sem, in_sem, out_sem, p_recv, p_send,
    id_send, id_recv, f_send, f_recv, ac_send, ac_recv, bx_send, bx_recv, cz_send, cz_recv,
    sib_send, sib_recv, y_send, y_recv,
):
    micros, sections, nx, nz, features = dims
    section = lax.axis_index("section")
    px = lax.axis_index("owner_0")
    pz = lax.axis_index("owner_1")
    pc = lax.axis_index("owner_2")
    chunks = micros * sections
    rows = pre_v.shape[0] // chunks
    hidden = w_v.shape[0]
    lanes = emb_v.shape[1]
    last = section == sections - 1

    def part(ref, t, size):
        return ref.at[pl.ds(pl.multiple_of(t * size, size), size)]

    def pre_copy(t):
        return pltpu.make_async_copy(part(pre_hbm, t, rows), part(pre_v, t, rows), pre_sem.at[t])

    def cot_copy(t):
        return pltpu.make_async_copy(part(cot_hbm, t, rows), part(rbuf, t, rows), in_sem.at[t])

    def remote(src, dst, send, recv, where):
        return pltpu.make_async_remote_copy(
            src_ref=src, dst_ref=dst, send_sem=send, recv_sem=recv,
            device_id=where, device_id_type=MESH,
        )

    def down_copy(t):
        return remote(
            part(sbuf, t, rows), part(rbuf, t, rows), out_sem.at[t], in_sem.at[t],
            {"section": lax.rem(section + sections - 1, sections)},
        )

    def p_copy(t):
        return remote(
            part(sbuf, t, rows), part(pbuf, t // sections, rows),
            p_send.at[t], p_recv.at[t // sections], {"section": lax.rem(t, sections)},
        )

    def chip(n):
        dx = lax.rem(n, nx)
        k = n // nx
        dz = ((k + 1) // 2) * (2 * lax.rem(k, 2) - 1)
        return lax.rem(px + dx, nx), lax.rem(pz + dz + nz, nz)

    w_copy = pltpu.make_async_copy(w_hbm, w_v, w_sem)
    x_copy = pltpu.make_async_copy(x_hbm, x_v, x_sem)
    emb_copy = pltpu.make_async_copy(emb_hbm, emb_v, emb_sem)
    ids_copy = pltpu.make_async_copy(ids_hbm, ids_v, ids_sem)
    w_copy.start()

    def begin(t, carry):
        pre_copy(t).start()

        @pl.when(last)
        def _():
            cot_copy(t).start()
        return carry

    lax.fori_loop(0, chunks, begin, 0)
    ids_copy.start()
    emb_copy.start()
    x_copy.start()

    barrier = pltpu.get_barrier_semaphore()
    for d in range(1, sections):
        pl.semaphore_signal(
            barrier, inc=1, device_id={"section": lax.rem(section + d, sections)},
            device_id_type=MESH,
        )

    def greet(n, carry):
        tx, tz = chip(n)

        def hail(core):
            pl.semaphore_signal(
                barrier, inc=1, device_id={"owner_0": tx, "owner_1": tz, "owner_2": core},
                device_id_type=MESH,
            )

        hail(1 - pc)

        @pl.when(n > 0)
        def _():
            hail(pc)
        return carry

    lax.fori_loop(0, nx * nz, greet, 0)

    across = lax.broadcasted_iota(jnp.int32, (128, hidden), 1)
    flipped = lax.rem(across, features) * features + across // features

    def make_fold(b, carry):
        down = lax.broadcasted_iota(jnp.int32, (128, hidden), 0) + b * 128
        value = jnp.where(down == across, 1.0, 0.0) + jnp.where(down == flipped, 1.0, 0.0)
        part(fold, b, 128)[...] = value.astype(BF16)
        return carry

    lax.fori_loop(0, hidden // 128, make_fold, 0)
    wide = GROUP * features
    for j in range(128 // features):
        down = lax.broadcasted_iota(jnp.int32, (128, wide), 0)
        col = lax.rem(lax.broadcasted_iota(jnp.int32, (128, wide), 1), features) + j * features
        pick[j] = jnp.where(down == col, 1.0, 0.0).astype(BF16)
    acc[...] = jnp.zeros_like(acc)

    pl.semaphore_wait(barrier, sections - 1 + 2 * nx * nz - 1)
    ids_copy.wait()

    def send_ids(n, carry):
        tx, tz = chip(n)
        mine = (px * nz + pz) * 2 + pc
        for r in range(2):
            there = (tx * nz + tz) * 2 + r
            home = (n == 0) & (pc == r)

            @pl.when(home)
            def _():
                pltpu.make_async_copy(ids_v.at[there], idr.at[mine], id_recv).start()

            @pl.when(jnp.logical_not(home))
            def _():
                remote(
                    ids_v.at[there], idr.at[mine], id_send, id_recv,
                    {"owner_0": tx, "owner_1": tz, "owner_2": r},
                ).start()
        return carry

    lax.fori_loop(0, nx * nz, send_ids, 0)
    w_copy.wait()

    def chain_step(t):
        pre_copy(t).wait()

        @pl.when(last)
        def _():
            cot_copy(t).wait()

        @pl.when(jnp.logical_not(last))
        def _():
            down_copy(t).wait_recv()

        at = pl.ds(pl.multiple_of(t * rows, rows), rows)
        incoming = rbuf[at, :]
        slope = jnp.where(pre_v[at, :] > 0, incoming, jnp.zeros_like(incoming))
        slopes[at, :] = slope
        sbuf[at, :] = dot(slope, w_v[...], NT).astype(BF16)

        @pl.when(section > 0)
        def _():
            down_copy(t).start()

        @pl.when((section == 0) & (lax.rem(t, sections) > 0))
        def _():
            p_copy(t).start()

        @pl.when((section == 0) & (lax.rem(t, sections) == 0))
        def _():
            own = pl.multiple_of((t // sections) * rows, rows)
            pbuf[pl.ds(own, rows), :] = sbuf[at, :]

    block = 256

    def weight_step(m):
        size = rows * sections
        at = pl.ds(pl.multiple_of(m * size, size), size)

        def column(b, carry):
            cols = pl.ds(pl.multiple_of(b * block, block), block)
            grown = dot(x_v[at, cols], slopes[at, :], TN)
            spot = pl.ds(b * (block // 32), block // 32)
            grown = grown.reshape(block // 32, 2, 16, hidden)

            @pl.when(m == 0)
            def _():
                wacc[spot] = grown

            @pl.when(m > 0)
            def _():
                wacc[spot] = wacc[spot] + grown
            return carry

        lax.fori_loop(0, hidden // block, column, 0)

    sibling = {"owner_2": 1 - pc}
    core_copy = remote(wacc.at[:, 1 - pc], wrecv, ac_send, ac_recv, sibling)

    def x_send(d):
        to = lax.rem(px + d, nx)
        return remote(part(wx, to, nz), wxr.at[d - 1], bx_send.at[d - 1], bx_recv.at[d - 1],
                      {"owner_0": to})

    def z_send(d):
        to = lax.rem(pz + d, nz)
        return remote(wz.at[to], wzr.at[d - 1], cz_send.at[d - 1], cz_recv.at[d - 1],
                      {"owner_1": to})

    def weight_x():
        core_copy.wait_recv()

        def join(k, carry):
            wx[k] = (wacc[k, pc] + wrecv[k]).astype(BF16)
            return carry

        lax.fori_loop(0, nx * nz, join, 0)
        for d in range(1, nx):
            x_send(d).start()

    def weight_z():
        for d in range(1, nx):
            x_send(d).wait_recv()

        def join(k, carry):
            total = wx[px * nz + k].astype(F32)
            for d in range(nx - 1):
                total = total + wxr[d, k].astype(F32)
            wz[k] = total.astype(BF16)
            return carry

        lax.fori_loop(0, nz, join, 0)
        for d in range(1, nz):
            z_send(d).start()

    def weight_end():
        total = wz[pz].astype(F32)
        for d in range(1, nz):
            z_send(d).wait_recv()
            total = total + wzr[d - 1].astype(F32)
        wg_out[...] = total * scale

    def feature_step(i):
        @pl.when(i == 0)
        def _():
            emb_copy.wait()

        @pl.when(section > 0)
        def _():
            p_copy(i * sections).wait_recv()

        p = pbuf[pl.ds(pl.multiple_of(i * rows, rows), rows), :]
        s = dot(p, fold[...], NN).astype(BF16)
        blocks = hidden // 128
        tall = jnp.concatenate([s[:, 128 * b:128 * b + 128] for b in range(blocks)], axis=0)
        per = 128 // features
        own_row = lax.rem(lax.broadcasted_iota(jnp.int32, (rows, wide), 0), GROUP)
        own_lane = lax.broadcasted_iota(jnp.int32, (rows, wide), 1) // features
        for j in range(per):
            e = dot(tall, pick[j], NN)
            for b in range(blocks):
                kept = jnp.where(own_row == own_lane, e[rows * b:rows * b + rows], 0.0)
                spread[b * per + j] = kept.astype(BF16)
        for g in range(rows // GROUP):
            lhs = spread[:, GROUP * g:GROUP * g + GROUP, :].reshape(features * GROUP, wide)
            at = pl.multiple_of((i * (rows // GROUP) + g) * wide, wide)
            out = dot(lhs, emb_v[pl.ds(at, wide), :], NN)
            fg[i, :, GROUP * g:GROUP * g + GROUP, :] = out.astype(BF16).reshape(features, GROUP, lanes)

        core = lax.rem(i, 2)
        slot = pl.ds(pl.multiple_of((pz * 2 + pc) * rows, rows), rows)

        def send(n, carry):
            tx, tz = chip(n)
            src = fg.at[i, tx * nz + tz]
            dst = arr.at[i // 2, px, slot]
            home = (n == 0) & (pc == core)

            @pl.when(home)
            def _():
                pltpu.make_async_copy(src, dst, f_recv.at[i // 2, px]).start()

            @pl.when(jnp.logical_not(home))
            def _():
                remote(src, dst, f_send.at[i], f_recv.at[i // 2, px],
                       {"owner_0": tx, "owner_1": tz, "owner_2": core}).start()
            return carry

        lax.fori_loop(0, nx * nz, send, 0)

    table_rows = acc.shape[0]

    def table_step(i):
        h = i // 2

        @pl.when(h == 0)
        def _():
            pltpu.make_async_copy(idr, idr, id_recv).wait()

        row = lax.broadcasted_iota(jnp.int32, (table_rows, 2 * rows), 0)

        def gather(g, carry):
            pltpu.make_async_copy(arr.at[h, g], arr.at[h, g], f_recv.at[h, g]).wait()
            for z in range(nz):
                both = idr[(g * nz + z) * 2] + idr[(g * nz + z) * 2 + 1]
                ids = jnp.where(h == 0, both[:, :2 * rows], both[:, 2 * rows:])
                onehot[:, z * 2 * rows:(z + 1) * 2 * rows] = jnp.where(row == ids, 1.0, 0.0).astype(BF16)
            acc[...] = acc[...] + dot(onehot[...], arr[h, g], NN)
            return carry

        lax.fori_loop(0, nx, gather, 0)

    first = jnp.where(last, chunks + 1, jnp.where(section == 0, 0, 4 * section + 1))
    ends = chunks + 1 + 4 * micros + 8

    def tick(now, carry):
        @pl.when(now < chunks)
        def _():
            chain_step(now)

        @pl.when((now < chunks) & (lax.rem(now, sections) == sections - 1))
        def _():
            @pl.when(now == sections - 1)
            def _():
                x_copy.wait()
            weight_step(now // sections)

        @pl.when(now == chunks)
        def _():
            core_copy.start()

        @pl.when(now == chunks + 1)
        def _():
            weight_x()

        lag = now - first

        @pl.when((lag >= 0) & (lax.rem(lag, 4) == 0) & (lag < 4 * micros))
        def _():
            feature_step(lag // 4)

        late = lag - 7

        @pl.when((late >= 0) & (lax.rem(late, 4) == 0) & (late < 4 * micros) & (lax.rem(late // 4, 2) == pc))
        def _():
            table_step(late // 4)

        @pl.when(now == chunks + 4)
        def _():
            weight_z()

        @pl.when(now == chunks + 8)
        def _():
            weight_end()
        return carry

    lax.fori_loop(0, ends, tick, 0)

    half = table_rows // 2
    sib_copy = remote(part(acc, 1 - pc, half), sib, sib_send, sib_recv, sibling)
    sib_copy.start()
    sib_copy.wait()
    mine = pl.ds(pl.multiple_of(pc * half, half), half)
    sib[...] = sib[...] + acc[mine, :]
    piece = half // sections

    def y_copy(d):
        to = lax.rem(section + d, sections)
        return remote(part(sib, to, piece), yrecv.at[d - 1], y_send.at[d - 1], y_recv.at[d - 1],
                      {"section": to})

    for d in range(1, sections):
        y_copy(d).start()
    total = part(sib, section, piece)[...]
    for d in range(1, sections):
        y_copy(d).wait_recv()
        total = total + yrecv[d - 1]
    tg_out[...] = total * scale

    def finish(t, carry):
        @pl.when(section > 0)
        def _():
            down_copy(t).wait_send()

        @pl.when((section == 0) & (lax.rem(t, sections) > 0))
        def _():
            p_copy(t).wait_send()
        return carry

    lax.fori_loop(0, chunks, finish, 0)
    some = pl.ds(0, 2 * nx * nz - 1)
    pltpu.make_async_copy(ids_v.at[some], ids_v.at[some], id_send).wait()
    for i in range(micros):
        @pl.when(pc == i % 2)
        def _():
            sent = fg.at[i, pl.ds(0, features - 1)]
            pltpu.make_async_copy(sent, sent, f_send.at[i]).wait()

        @pl.when(pc != i % 2)
        def _():
            sent = fg.at[i]
            pltpu.make_async_copy(sent, sent, f_send.at[i]).wait()
    core_copy.wait_send()
    for d in range(1, nx):
        x_send(d).wait_send()
    for d in range(1, nz):
        z_send(d).wait_send()
    for d in range(1, sections):
        y_copy(d).wait_send()


def per_device(weights, inputs, preact, cotangent, embeddings, row_ids):
    sections = lax.axis_size("section")
    nx, nz, cores = (lax.axis_size(a) for a in OWNER)
    micros, batch_rows, hidden = cotangent.shape
    quarter, features, width = embeddings.shape[1:]
    total = micros * batch_rows
    owners = nx * nz * cores
    scale = 1.0 / math.sqrt(total * owners)
    table_rows = 1024
    ids = jnp.transpose(row_ids, (2, 0, 1)).reshape(features, micros // 2, 2, quarter)
    ids = jnp.transpose(ids, (0, 2, 1, 3))[:, :, :, None, :]
    core = lax.axis_index("owner_2")
    ids = jnp.where(jnp.arange(2).reshape(1, 1, 1, 2, 1) == core, ids, 0)
    ids = ids.reshape(owners, 1, 2 * cores * quarter)
    dma = pltpu.SemaphoreType.DMA
    vmem = pl.BlockSpec(memory_space=pltpu.VMEM)
    hbm = pl.BlockSpec(memory_space=pl.ANY)
    chunks = micros * sections
    rows = total // chunks
    wide = GROUP * features
    part = hidden // owners
    half = table_rows // 2
    V = pltpu.VMEM
    weight_grad, table_grad = pl.pallas_call(
        functools.partial(step_kernel, (micros, sections, nx, nz, features), scale),
        out_shape=(
            jax.ShapeDtypeStruct((part, hidden), F32),
            jax.ShapeDtypeStruct((half // sections, width), F32),
        ),
        in_specs=[hbm] * 6,
        out_specs=(vmem, vmem),
        scratch_shapes=[
            V((hidden, hidden), BF16),
            V((total, hidden), BF16),
            V((total, hidden), BF16),
            V((micros * quarter * features, width), BF16),
            V(ids.shape, jnp.int32),
            V((total, hidden), BF16),
            V((total, hidden), BF16),
            V((total, hidden), BF16),
            V((micros * quarter, hidden), BF16),
            V((nx * nz, 2, part, hidden), F32),
            V((nx * nz, part, hidden), F32),
            V((nx * nz, part, hidden), BF16),
            V((nx - 1, nz, part, hidden), BF16),
            V((nz, part, hidden), BF16),
            V((nz - 1, part, hidden), BF16),
            V((hidden, hidden), BF16),
            V((128 // features, 128, wide), BF16),
            V((features, rows, wide), BF16),
            V((micros, features, rows, width), BF16),
            V((micros // 2, nx, nz * 2 * rows, width), BF16),
            V(ids.shape, jnp.int32),
            V((table_rows, nz * 2 * rows), BF16),
            V((table_rows, width), F32),
            V((half, width), F32),
            V((sections - 1, half // sections, width), F32),
            dma, dma, dma((chunks,)), dma, dma, dma((chunks,)), dma((chunks,)),
            dma((micros,)), dma((chunks,)),
            dma, dma, dma((micros,)), dma((micros // 2, nx)),
            dma, dma, dma((nx - 1,)), dma((nx - 1,)), dma((nz - 1,)), dma((nz - 1,)),
            dma, dma, dma((sections - 1,)), dma((sections - 1,)),
        ],
        compiler_params=pltpu.CompilerParams(
            collective_id=0, has_side_effects=True, vmem_limit_bytes=60 * 1024 * 1024
        ),
    )(
        weights[0],
        inputs.reshape(total, hidden),
        preact.reshape(total, hidden),
        cotangent.reshape(total, hidden),
        embeddings.reshape(micros * quarter * features, width),
        ids,
    )
    return (weight_grad[None], table_grad[None])


def solution(mesh):
    finer = Mesh(
        mesh.devices.reshape(mesh.shape["section"], 4, 8, 2),
        ("section", "owner_0", "owner_1", "owner_2"),
    )
    placed = (
        P("section", None, None),
        P("section", None, OWNER, None),
        P("section", None, OWNER, None),
        P(None, OWNER, None),
        P(None, OWNER_SECTION, None, None),
        P(None, OWNER_SECTION, None),
    )
    return jax.shard_map(
        per_device,
        mesh=finer,
        in_specs=placed,
        out_specs=(P("section", OWNER, None), P(OWNER, "section", None)),
        check_vma=False,
    )
```

```python
import functools
import math

import jax
import jax.numpy as jnp
from jax import lax
from jax.experimental import pallas as pl
from jax.experimental.pallas import tpu as pltpu
from jax.sharding import Mesh
from jax.sharding import PartitionSpec as P

OWNER = ("owner_0", "owner_1", "owner_2")
OWNER_SECTION = ("owner_0", "owner_1", "owner_2", "section")
MESH = pl.DeviceIdType.MESH
BF16 = jnp.bfloat16
F32 = jnp.float32
NN = (((1,), (0,)), ((), ()))
NT = (((1,), (1,)), ((), ()))
TN = (((0,), (0,)), ((), ()))
GROUP = 16


def dot(a, b, dims):
    return lax.dot_general(a, b, dims, preferred_element_type=F32)


def step_kernel(
    dims, scale,
    w_hbm, x_hbm, pre_hbm, cot_hbm, emb_hbm, ids_hbm,
    wg_out, tg_out,
    w_v, wt_v, x_v, pre_v, emb_v, ids_v, rbuf, sbuf, slopes, pbuf, wacc, wsend, wrecv, wx, wxr, wz, wzr,
    fold, pick, spread, fg, arr, idr, onehot, acc, sib, ysend, yrecv,
    near, w_sem, x_sem, pre_sem, emb_sem, ids_sem, in_sem, out_sem, p_recv, p_send,
    id_send, id_recv, f_send, f_recv, ac_send, ac_recv, bx_send, bx_recv, cz_send, cz_recv,
    sib_send, sib_recv, y_send, y_recv,
):
    micros, sections, nx, nz, features = dims
    section = lax.axis_index("section")
    px = lax.axis_index("owner_0")
    pz = lax.axis_index("owner_1")
    pc = lax.axis_index("owner_2")
    rows = pre_v.shape[0] // (micros * sections)
    fine = rows // 2
    small = 2 * sections
    chunks = small + (micros - 1) * sections
    hidden = w_v.shape[0]
    lanes = emb_v.shape[1]
    last = section == sections - 1

    def part(ref, t, size):
        return ref.at[pl.ds(pl.multiple_of(t * size, size), size)]

    def spot(t, size):
        start = t * fine if size == fine else small * fine + (t - small) * rows
        return pl.ds(pl.multiple_of(start, fine), size)

    def each_chunk(body):
        def narrow(t, carry):
            body(t, fine)
            return carry

        def broad(t, carry):
            body(t, rows)
            return carry

        lax.fori_loop(0, small, narrow, 0)
        lax.fori_loop(small, chunks, broad, 0)

    def pre_copy(t, size):
        at = spot(t, size)
        return pltpu.make_async_copy(pre_hbm.at[at], pre_v.at[at], pre_sem.at[t])

    def cot_copy(t, size):
        at = spot(t, size)
        return pltpu.make_async_copy(cot_hbm.at[at], rbuf.at[at], in_sem.at[t])

    def remote(src, dst, send, recv, where):
        return pltpu.make_async_remote_copy(
            src_ref=src, dst_ref=dst, send_sem=send, recv_sem=recv,
            device_id=where, device_id_type=MESH,
        )

    def down_copy(t, size):
        at = spot(t, size)
        return remote(
            sbuf.at[at], rbuf.at[at], out_sem.at[t], in_sem.at[t],
            {"section": lax.rem(section + sections - 1, sections)},
        )

    def p_place(t, size):
        if size == fine:
            return t // 2, 0, lax.rem(t, 2) * fine
        unit = (t - small) // sections + 1
        return lax.rem(t, sections), unit, unit * rows

    def p_copy(t, size):
        to, unit, start = p_place(t, size)
        return remote(
            sbuf.at[spot(t, size)], pbuf.at[pl.ds(pl.multiple_of(start, fine), size)],
            p_send.at[t], p_recv.at[unit], {"section": to},
        )

    def chip(n):
        dx = lax.rem(n, nx)
        k = n // nx
        dz = ((k + 1) // 2) * (2 * lax.rem(k, 2) - 1)
        return lax.rem(px + dx, nx), lax.rem(pz + dz + nz, nz)

    w_copy = pltpu.make_async_copy(w_hbm, w_v, w_sem)
    x_copy = pltpu.make_async_copy(x_hbm, x_v, x_sem)
    emb_copy = pltpu.make_async_copy(emb_hbm, emb_v, emb_sem)
    ids_copy = pltpu.make_async_copy(ids_hbm, ids_v, ids_sem)
    w_copy.start()

    def begin(t, size):
        pre_copy(t, size).start()

        @pl.when(last)
        def _():
            cot_copy(t, size).start()

    each_chunk(begin)
    ids_copy.start()
    emb_copy.start()
    x_copy.start()

    barrier = pltpu.get_barrier_semaphore()

    def peers(name, place, count, sem):
        for d in range(1, count):
            pl.semaphore_signal(
                sem, inc=1, device_id={name: lax.rem(place + d, count)}, device_id_type=MESH
            )

    inner = (("owner_1", pz, nz), ("owner_0", px, nx), ("owner_2", pc, 2))
    peers("section", section, sections, barrier)

    @pl.when(section == 0)
    def _():
        for name, place, count in inner:
            peers(name, place, count, barrier)
        pl.semaphore_wait(barrier, sections - 1 + sum(count - 1 for name, place, count in inner))

    @pl.when(section > 0)
    def _():
        pl.semaphore_wait(barrier, sections - 1)

    wide = GROUP * features

    def prepare():
        across = lax.broadcasted_iota(jnp.int32, (128, hidden), 1)
        flipped = lax.rem(across, features) * features + across // features

        def make_fold(b, carry):
            down = lax.broadcasted_iota(jnp.int32, (128, hidden), 0) + b * 128
            value = jnp.where(down == across, 1.0, 0.0) + jnp.where(down == flipped, 1.0, 0.0)
            part(fold, b, 128)[...] = value.astype(BF16)
            return carry

        lax.fori_loop(0, hidden // 128, make_fold, 0)
        for j in range(128 // features):
            down = lax.broadcasted_iota(jnp.int32, (128, wide), 0)
            col = lax.rem(lax.broadcasted_iota(jnp.int32, (128, wide), 1), features) + j * features
            pick[j] = jnp.where(down == col, 1.0, 0.0).astype(BF16)
        acc[...] = jnp.zeros_like(acc)

    def send_ids(n, carry):
        tx, tz = chip(n)
        mine = (px * nz + pz) * 2 + pc
        for r in range(2):
            there = (tx * nz + tz) * 2 + r
            home = (n == 0) & (pc == r)

            @pl.when(home)
            def _():
                pltpu.make_async_copy(ids_v.at[there], idr.at[mine], id_recv).start()

            @pl.when(jnp.logical_not(home))
            def _():
                remote(
                    ids_v.at[there], idr.at[mine], id_send, id_recv,
                    {"owner_0": tx, "owner_1": tz, "owner_2": r},
                ).start()
        return carry

    @pl.when(section == 0)
    def _():
        peers(*inner[0], near.at[0])

    def meet(stage):
        pl.semaphore_wait(near.at[stage], inner[stage][2] - 1)
        if stage < 2:
            peers(*inner[stage + 1], near.at[stage + 1])
        else:
            peers("section", section, sections, near.at[3])

    def exchange_ids():
        @pl.when(section > 0)
        def _():
            pl.semaphore_wait(near.at[3], 1)

        ids_copy.wait()
        lax.fori_loop(0, nx * nz, send_ids, 0)

    w_copy.wait()

    @pl.when(jnp.logical_not(last))
    def _():
        def turn(b, carry):
            cols = pl.ds(pl.multiple_of(b * 128, 128), 128)
            wt_v[:, cols] = part(w_v, b, 128)[...].T
            return carry

        lax.fori_loop(0, hidden // 128, turn, 0)
        prepare()

    def chain_step(t, size):
        pre_copy(t, size).wait()

        @pl.when(last)
        def _():
            cot_copy(t, size).wait()

        @pl.when(jnp.logical_not(last))
        def _():
            down_copy(t, size).wait_recv()

        at = spot(t, size)
        incoming = rbuf[at, :]
        slope = jnp.where(pre_v[at, :] > 0, incoming, jnp.zeros_like(incoming))
        slopes[at, :] = slope

        @pl.when(last)
        def _():
            sbuf[at, :] = dot(slope, w_v[...], NT).astype(BF16)

        @pl.when(jnp.logical_not(last))
        def _():
            sbuf[at, :] = dot(slope, wt_v[...], NN).astype(BF16)

        @pl.when(section > 0)
        def _():
            down_copy(t, size).start()

        to, unit, start = p_place(t, size)

        @pl.when((section == 0) & (to > 0))
        def _():
            p_copy(t, size).start()

        @pl.when((section == 0) & (to == 0))
        def _():
            pbuf[pl.ds(pl.multiple_of(start, fine), size), :] = sbuf[at, :]

    block = 256

    def weight_step(m):
        size = rows * sections
        at = pl.ds(pl.multiple_of(m * size, size), size)

        def column(b, carry):
            cols = pl.ds(pl.multiple_of(b * block, block), block)
            grown = dot(x_v[at, cols], slopes[at, :], TN)
            spot = pl.ds(b * (block // 32), block // 32)
            grown = grown.reshape(block // 32, 2, 16, hidden)

            @pl.when(m == 0)
            def _():
                wacc[spot] = grown

            @pl.when(m > 0)
            def _():
                wacc[spot] = wacc[spot] + grown
            return carry

        lax.fori_loop(0, hidden // block, column, 0)

    sibling = {"owner_2": 1 - pc}
    core_copy = remote(wsend, wrecv, ac_send, ac_recv, sibling)

    def weight_core():
        def cast(k, carry):
            wsend[k] = wacc[k, 1 - pc].astype(BF16)
            return carry

        lax.fori_loop(0, nx * nz, cast, 0)
        core_copy.start()

    def x_send(d):
        to = lax.rem(px + d, nx)
        return remote(part(wx, to, nz), wxr.at[d - 1], bx_send.at[d - 1], bx_recv.at[d - 1],
                      {"owner_0": to})

    def z_send(d):
        to = lax.rem(pz + d, nz)
        return remote(wz.at[to], wzr.at[d - 1], cz_send.at[d - 1], cz_recv.at[d - 1],
                      {"owner_1": to})

    def weight_x():
        core_copy.wait_recv()

        def join(k, carry):
            wx[k] = (wacc[k, pc] + wrecv[k].astype(F32)).astype(BF16)
            return carry

        lax.fori_loop(0, nx * nz, join, 0)
        for d in range(1, nx):
            x_send(d).start()

    def weight_z():
        for d in range(1, nx):
            x_send(d).wait_recv()

        def join(k, carry):
            total = wx[px * nz + k].astype(F32)
            for d in range(nx - 1):
                total = total + wxr[d, k].astype(F32)
            wz[k] = total.astype(BF16)
            return carry

        lax.fori_loop(0, nz, join, 0)
        for d in range(1, nz):
            z_send(d).start()

    def weight_end():
        total = wz[pz].astype(F32)
        for d in range(1, nz):
            z_send(d).wait_recv()
            total = total + wzr[d - 1].astype(F32)
        wg_out[...] = total * scale

    def feature_step(i):
        @pl.when(i == 0)
        def _():
            emb_copy.wait()

        @pl.when(section > 0)
        def _():
            here = part(pbuf, i, rows)
            pltpu.make_async_copy(here, here, p_recv.at[i]).wait()

        p = pbuf[pl.ds(pl.multiple_of(i * rows, rows), rows), :]
        s = dot(p, fold[...], NN).astype(BF16)
        blocks = hidden // 128
        tall = jnp.concatenate([s[:, 128 * b:128 * b + 128] for b in range(blocks)], axis=0)
        per = 128 // features
        own_row = lax.rem(lax.broadcasted_iota(jnp.int32, (rows, wide), 0), GROUP)
        own_lane = lax.broadcasted_iota(jnp.int32, (rows, wide), 1) // features
        for j in range(per):
            e = dot(tall, pick[j], NN)
            for b in range(blocks):
                kept = jnp.where(own_row == own_lane, e[rows * b:rows * b + rows], 0.0)
                spread[b * per + j] = kept.astype(BF16)
        for g in range(rows // GROUP):
            lhs = spread[:, GROUP * g:GROUP * g + GROUP, :].reshape(features * GROUP, wide)
            at = pl.multiple_of((i * (rows // GROUP) + g) * wide, wide)
            out = dot(lhs, emb_v[pl.ds(at, wide), :], NN)
            fg[i, :, GROUP * g:GROUP * g + GROUP, :] = out.astype(BF16).reshape(features, GROUP, lanes)

        core = lax.rem(i, 2)
        slot = pl.ds(pl.multiple_of((pz * 2 + pc) * rows, rows), rows)

        def send(n, carry):
            tx, tz = chip(n)
            src = fg.at[i, tx * nz + tz]
            dst = arr.at[i // 2, px, slot]
            home = (n == 0) & (pc == core)

            @pl.when(home)
            def _():
                pltpu.make_async_copy(src, dst, f_recv.at[i // 2, px]).start()

            @pl.when(jnp.logical_not(home))
            def _():
                remote(src, dst, f_send.at[i], f_recv.at[i // 2, px],
                       {"owner_0": tx, "owner_1": tz, "owner_2": core}).start()
            return carry

        lax.fori_loop(0, nx * nz, send, 0)

    table_rows = acc.shape[0]

    def table_step(i):
        h = i // 2

        @pl.when(h == 0)
        def _():
            pltpu.make_async_copy(idr, idr, id_recv).wait()

        row = lax.broadcasted_iota(jnp.int32, (table_rows, 2 * rows), 0)

        def gather(g, carry):
            pltpu.make_async_copy(arr.at[h, g], arr.at[h, g], f_recv.at[h, g]).wait()
            for z in range(nz):
                both = idr[(g * nz + z) * 2] + idr[(g * nz + z) * 2 + 1]
                ids = jnp.where(h == 0, both[:, :2 * rows], both[:, 2 * rows:])
                onehot[:, z * 2 * rows:(z + 1) * 2 * rows] = jnp.where(row == ids, 1.0, 0.0).astype(BF16)
            acc[...] = acc[...] + dot(onehot[...], arr[h, g], NN)
            return carry

        lax.fori_loop(0, nx, gather, 0)

    def by_section(*values):
        chosen = values[-1]
        for n in range(sections - 1):
            chosen = jnp.where(section == n, values[n], chosen)
        return chosen

    features_at = (
        by_section(7, 9, 12, 21), by_section(9, 13, 16, 26),
        by_section(12, 17, 20, 30), by_section(16, 20, 22, 34),
    )
    tables_at = (
        by_section(14, 21, 21, 31), by_section(21, 21, 23, 35),
        by_section(21, 22, 24, 36), by_section(22, 24, 25, 37),
    )
    meet_time = by_section(7, 9, 12, 19)
    x_time = by_section(20, 21, 21, 22)
    z_time = by_section(23, 23, 23, 27)
    ends = 38

    def tick(now, carry):
        for stage in range(3):
            @pl.when((section == 0) & (now == stage))
            def _():
                meet(stage)

        @pl.when(now < small)
        def _():
            chain_step(now, fine)

        @pl.when((now >= small) & (now < chunks))
        def _():
            chain_step(now, rows)

        @pl.when(now == meet_time)
        def _():
            exchange_ids()

        @pl.when(last & (now == 6))
        def _():
            prepare()

        done = now + 1 - small

        @pl.when((now < chunks) & (done >= 0) & (lax.rem(done, sections) == 0))
        def _():
            @pl.when(done == 0)
            def _():
                x_copy.wait()
            weight_step(done // sections)

        @pl.when(now == chunks)
        def _():
            weight_core()

        which = micros
        for n in range(micros):
            which = jnp.where(now == features_at[n], n, which)

        @pl.when(which < micros)
        def _():
            feature_step(which)

        @pl.when(now == x_time)
        def _():
            weight_x()

        @pl.when(now == z_time)
        def _():
            weight_z()

        unit = micros
        for n in range(micros):
            unit = jnp.where((now == tables_at[n]) & (pc == n % 2), n, unit)

        @pl.when(unit < micros)
        def _():
            table_step(unit)
        return carry

    lax.fori_loop(0, ends, tick, 0)

    half = table_rows // 2
    sib_copy = remote(part(acc, 1 - pc, half), sib, sib_send, sib_recv, sibling)
    sib_copy.start()
    sib_copy.wait()
    mine = pl.ds(pl.multiple_of(pc * half, half), half)
    sib[...] = sib[...] + acc[mine, :]
    ysend[...] = sib[...].astype(BF16)
    piece = half // sections

    def y_copy(d):
        to = lax.rem(section + d, sections)
        return remote(part(ysend, to, piece), yrecv.at[d - 1], y_send.at[d - 1], y_recv.at[d - 1],
                      {"section": to})

    for d in range(1, sections):
        y_copy(d).start()
    weight_end()
    total = part(sib, section, piece)[...]
    for d in range(1, sections):
        y_copy(d).wait_recv()
        total = total + yrecv[d - 1].astype(F32)
    tg_out[...] = total * scale

    def finish(t, size):
        @pl.when(section > 0)
        def _():
            down_copy(t, size).wait_send()

        @pl.when((section == 0) & (p_place(t, size)[0] > 0))
        def _():
            p_copy(t, size).wait_send()

    each_chunk(finish)
    some = pl.ds(0, 2 * nx * nz - 1)
    pltpu.make_async_copy(ids_v.at[some], ids_v.at[some], id_send).wait()
    for i in range(micros):
        @pl.when(pc == i % 2)
        def _():
            sent = fg.at[i, pl.ds(0, features - 1)]
            pltpu.make_async_copy(sent, sent, f_send.at[i]).wait()

        @pl.when(pc != i % 2)
        def _():
            sent = fg.at[i]
            pltpu.make_async_copy(sent, sent, f_send.at[i]).wait()
    core_copy.wait_send()
    for d in range(1, nx):
        x_send(d).wait_send()
    for d in range(1, nz):
        z_send(d).wait_send()
    for d in range(1, sections):
        y_copy(d).wait_send()


def per_device(weights, inputs, preact, cotangent, embeddings, row_ids):
    sections = lax.axis_size("section")
    nx, nz, cores = (lax.axis_size(a) for a in OWNER)
    micros, batch_rows, hidden = cotangent.shape
    quarter, features, width = embeddings.shape[1:]
    total = micros * batch_rows
    owners = nx * nz * cores
    scale = 1.0 / math.sqrt(total * owners)
    table_rows = 1024
    ids = jnp.transpose(row_ids, (2, 0, 1)).reshape(features, micros // 2, 2, quarter)
    ids = jnp.transpose(ids, (0, 2, 1, 3))[:, :, :, None, :]
    core = lax.axis_index("owner_2")
    ids = jnp.where(jnp.arange(2).reshape(1, 1, 1, 2, 1) == core, ids, 0)
    ids = ids.reshape(owners, 1, 2 * cores * quarter)
    dma = pltpu.SemaphoreType.DMA
    vmem = pl.BlockSpec(memory_space=pltpu.VMEM)
    hbm = pl.BlockSpec(memory_space=pl.ANY)
    chunks = (micros + 1) * sections
    rows = total // (micros * sections)
    wide = GROUP * features
    part = hidden // owners
    half = table_rows // 2
    V = pltpu.VMEM
    weight_grad, table_grad = pl.pallas_call(
        functools.partial(step_kernel, (micros, sections, nx, nz, features), scale),
        out_shape=(
            jax.ShapeDtypeStruct((part, hidden), F32),
            jax.ShapeDtypeStruct((half // sections, width), F32),
        ),
        in_specs=[hbm] * 6,
        out_specs=(vmem, vmem),
        scratch_shapes=[
            V((hidden, hidden), BF16),
            V((hidden, hidden), BF16),
            V((total, hidden), BF16),
            V((total, hidden), BF16),
            V((micros * quarter * features, width), BF16),
            V(ids.shape, jnp.int32),
            V((total, hidden), BF16),
            V((total, hidden), BF16),
            V((total, hidden), BF16),
            V((micros * quarter, hidden), BF16),
            V((nx * nz, 2, part, hidden), F32),
            V((nx * nz, part, hidden), BF16),
            V((nx * nz, part, hidden), BF16),
            V((nx * nz, part, hidden), BF16),
            V((nx - 1, nz, part, hidden), BF16),
            V((nz, part, hidden), BF16),
            V((nz - 1, part, hidden), BF16),
            V((hidden, hidden), BF16),
            V((128 // features, 128, wide), BF16),
            V((features, rows, wide), BF16),
            V((micros, features, rows, width), BF16),
            V((micros // 2, nx, nz * 2 * rows, width), BF16),
            V(ids.shape, jnp.int32),
            V((table_rows, nz * 2 * rows), BF16),
            V((table_rows, width), F32),
            V((half, width), F32),
            V((half, width), BF16),
            V((sections - 1, half // sections, width), BF16),
            pltpu.SemaphoreType.REGULAR((4,)),
            dma, dma, dma((chunks,)), dma, dma, dma((chunks,)), dma((chunks,)),
            dma((micros,)), dma((chunks,)),
            dma, dma, dma((micros,)), dma((micros // 2, nx)),
            dma, dma, dma((nx - 1,)), dma((nx - 1,)), dma((nz - 1,)), dma((nz - 1,)),
            dma, dma, dma((sections - 1,)), dma((sections - 1,)),
        ],
        compiler_params=pltpu.CompilerParams(
            collective_id=0, has_side_effects=True, vmem_limit_bytes=60 * 1024 * 1024
        ),
    )(
        weights[0],
        inputs.reshape(total, hidden),
        preact.reshape(total, hidden),
        cotangent.reshape(total, hidden),
        embeddings.reshape(micros * quarter * features, width),
        ids,
    )
    return (weight_grad[None], table_grad[None])


def solution(mesh):
    finer = Mesh(
        mesh.devices.reshape(mesh.shape["section"], 4, 8, 2),
        ("section", "owner_0", "owner_1", "owner_2"),
    )
    placed = (
        P("section", None, None),
        P("section", None, OWNER, None),
        P("section", None, OWNER, None),
        P(None, OWNER, None),
        P(None, OWNER_SECTION, None, None),
        P(None, OWNER_SECTION, None),
    )
    return jax.shard_map(
        per_device,
        mesh=finer,
        in_specs=placed,
        out_specs=(P("section", OWNER, None), P(OWNER, "section", None)),
        check_vma=False,
    )
```

```python
import functools
import math

import jax
import jax.numpy as jnp
from jax import lax
from jax.experimental import pallas as pl
from jax.experimental.pallas import tpu as pltpu
from jax.sharding import Mesh
from jax.sharding import PartitionSpec as P

OWNER = ("owner_0", "owner_1", "owner_2")
OWNER_SECTION = ("owner_0", "owner_1", "owner_2", "section")
MESH = pl.DeviceIdType.MESH
BF16 = jnp.bfloat16
F32 = jnp.float32
NN = (((1,), (0,)), ((), ()))
NT = (((1,), (1,)), ((), ()))
TN = (((0,), (0,)), ((), ()))
GROUP = 16


def dot(a, b, dims):
    return lax.dot_general(a, b, dims, preferred_element_type=F32)


def step_kernel(
    dims, scale,
    w_hbm, x_hbm, pre_hbm, cot_hbm, emb_hbm, ids_hbm,
    wg_out, tg_out,
    w_v, wt_v, x_v, pre_v, emb_v, raw_v, ids_v, rbuf, sbuf, slopes, pbuf, wacc, wsend, wrecv, wx, wxr, wz, wzr, vz, vzr, vx, vxr,
    fold, pick, spread, fg, arr, idr, onehot, acc, sib, ysend, yrecv, fsend, frecv,
    near, w_sem, x_sem, pre_sem, emb_sem, ids_sem, in_sem, out_sem, p_recv, p_send,
    id_send, id_recv, f_send, f_recv, ac_send, ac_recv, bx_send, bx_recv, cz_send, cz_recv, bz_send, bz_recv, cx_send, cx_recv,
    sib_send, sib_recv, y_send, y_recv, far_send, far_recv,
):
    micros, sections, nx, nz, features = dims
    section = lax.axis_index("section")
    px = lax.axis_index("owner_0")
    pz = lax.axis_index("owner_1")
    pc = lax.axis_index("owner_2")
    rows = pre_v.shape[0] // (micros * sections)
    fine = rows // 2
    small = 2 * sections
    chunks = small + (micros - 1) * sections
    hidden = w_v.shape[0]
    lanes = emb_v.shape[1]
    last = section == sections - 1

    def part(ref, t, size):
        return ref.at[pl.ds(pl.multiple_of(t * size, size), size)]

    def spot(t, size):
        start = t * fine if size == fine else small * fine + (t - small) * rows
        return pl.ds(pl.multiple_of(start, fine), size)

    def each_chunk(body):
        def narrow(t, carry):
            body(t, fine)
            return carry

        def broad(t, carry):
            body(t, rows)
            return carry

        lax.fori_loop(0, small, narrow, 0)
        lax.fori_loop(small, chunks, broad, 0)

    def pre_copy(t, size):
        at = spot(t, size)
        return pltpu.make_async_copy(pre_hbm.at[at], pre_v.at[at], pre_sem.at[t])

    def cot_copy(t, size):
        at = spot(t, size)
        return pltpu.make_async_copy(cot_hbm.at[at], rbuf.at[at], in_sem.at[t])

    def remote(src, dst, send, recv, where):
        return pltpu.make_async_remote_copy(
            src_ref=src, dst_ref=dst, send_sem=send, recv_sem=recv,
            device_id=where, device_id_type=MESH,
        )

    def down_copy(t, size):
        at = spot(t, size)
        return remote(
            sbuf.at[at], rbuf.at[at], out_sem.at[t], in_sem.at[t],
            {"section": lax.rem(section + sections - 1, sections)},
        )

    def p_place(t, size):
        if size == fine:
            return t // 2, 0, lax.rem(t, 2) * fine
        unit = (t - small) // sections + 1
        return lax.rem(t, sections), unit, unit * rows

    def p_copy(t, size):
        to, unit, start = p_place(t, size)
        return remote(
            sbuf.at[spot(t, size)], pbuf.at[pl.ds(pl.multiple_of(start, fine), size)],
            p_send.at[t], p_recv.at[unit], {"section": to},
        )

    def chip(n):
        dx = lax.rem(n, nx)
        k = n // nx
        dz = ((k + 1) // 2) * (2 * lax.rem(k, 2) - 1)
        return lax.rem(px + dx, nx), lax.rem(pz + dz + nz, nz)

    w_copy = pltpu.make_async_copy(w_hbm, w_v, w_sem)
    x_copy = pltpu.make_async_copy(x_hbm, x_v, x_sem)
    emb_copy = pltpu.make_async_copy(emb_hbm, emb_v, emb_sem)
    ids_copy = pltpu.make_async_copy(ids_hbm, raw_v, ids_sem)
    w_copy.start()

    def begin(t, size):
        pre_copy(t, size).start()

        @pl.when(last)
        def _():
            cot_copy(t, size).start()

    each_chunk(begin)
    ids_copy.start()
    emb_copy.start()
    x_copy.start()

    barrier = pltpu.get_barrier_semaphore()

    def peers(name, place, count, sem):
        for d in range(1, count):
            pl.semaphore_signal(
                sem, inc=1, device_id={name: lax.rem(place + d, count)}, device_id_type=MESH
            )

    inner = (("owner_1", pz, nz), ("owner_0", px, nx), ("owner_2", pc, 2))
    peers("section", section, sections, barrier)

    @pl.when(section == 0)
    def _():
        for name, place, count in inner:
            peers(name, place, count, barrier)
        pl.semaphore_wait(barrier, sections - 1 + sum(count - 1 for name, place, count in inner))

    @pl.when(section > 0)
    def _():
        pl.semaphore_wait(barrier, sections - 1)

    wide = GROUP * features

    def prepare():
        across = lax.broadcasted_iota(jnp.int32, (128, hidden), 1)
        flipped = lax.rem(across, features) * features + across // features

        def make_fold(b, carry):
            down = lax.broadcasted_iota(jnp.int32, (128, hidden), 0) + b * 128
            value = jnp.where(down == across, 1.0, 0.0) + jnp.where(down == flipped, 1.0, 0.0)
            part(fold, b, 128)[...] = value.astype(BF16)
            return carry

        lax.fori_loop(0, hidden // 128, make_fold, 0)
        for j in range(128 // features):
            down = lax.broadcasted_iota(jnp.int32, (128, wide), 0)
            col = lax.rem(lax.broadcasted_iota(jnp.int32, (128, wide), 1), features) + j * features
            pick[j] = jnp.where(down == col, 1.0, 0.0).astype(BF16)
        acc[...] = jnp.zeros_like(acc)
        ids_copy.wait()
        owner_lane = lax.rem(lax.broadcasted_iota(jnp.int32, (features, 4 * rows), 1) // rows, 2)
        for r in range(2):
            first, second = raw_v[r], raw_v[2 + r]
            spaced = jnp.concatenate([first, first, second, second], axis=1)
            spaced = jnp.where(owner_lane == pc, spaced, 0)
            for f in range(features):
                ids_v[f * 2 + r] = spaced[f:f + 1, :]

    near_z = nz // 2 + 1

    def gather_at(n):
        tx, tz = chip(n)
        k = n // nx
        far = k >= near_z
        home = (lax.rem(n, nx) == 0) & ((k == 0) | (k == nz - 1))
        return tx, lax.rem(tz + jnp.where(far, nz // 2, 0), nz), k, home, tx * nz + tz

    def send_ids(n, carry):
        tx, cz, k, own_chip, feature = gather_at(n)
        mine = (px * nz + k) * 2 + pc
        for r in range(2):
            there = feature * 2 + r
            home = own_chip & (pc == r)

            @pl.when(home)
            def _():
                pltpu.make_async_copy(ids_v.at[there], idr.at[mine], id_recv).start()

            @pl.when(jnp.logical_not(home))
            def _():
                remote(
                    ids_v.at[there], idr.at[mine], id_send, id_recv,
                    {"owner_0": tx, "owner_1": cz, "owner_2": r},
                ).start()
        return carry

    @pl.when(section == 0)
    def _():
        peers(*inner[0], near.at[0])

    def meet(stage):
        pl.semaphore_wait(near.at[stage], inner[stage][2] - 1)
        if stage < 2:
            peers(*inner[stage + 1], near.at[stage + 1])
        else:
            peers("section", section, sections, near.at[3])

    def exchange_ids():
        @pl.when(section > 0)
        def _():
            pl.semaphore_wait(near.at[3], 1)

        lax.fori_loop(0, nx * nz, send_ids, 0)

    w_copy.wait()

    @pl.when(jnp.logical_not(last))
    def _():
        def turn(b, carry):
            cols = pl.ds(pl.multiple_of(b * 128, 128), 128)
            wt_v[:, cols] = part(w_v, b, 128)[...].T
            return carry

        lax.fori_loop(0, hidden // 128, turn, 0)
        prepare()

    def chain_step(t, size):
        pre_copy(t, size).wait()

        @pl.when(last)
        def _():
            cot_copy(t, size).wait()

        @pl.when(jnp.logical_not(last))
        def _():
            down_copy(t, size).wait_recv()

        at = spot(t, size)
        incoming = rbuf[at, :]
        slope = jnp.where(pre_v[at, :] > 0, incoming, jnp.zeros_like(incoming))
        slopes[at, :] = slope

        @pl.when(last)
        def _():
            sbuf[at, :] = dot(slope, w_v[...], NT).astype(BF16)

        @pl.when(jnp.logical_not(last))
        def _():
            sbuf[at, :] = dot(slope, wt_v[...], NN).astype(BF16)

        @pl.when(section > 0)
        def _():
            down_copy(t, size).start()

        to, unit, start = p_place(t, size)

        @pl.when((section == 0) & (to > 0))
        def _():
            p_copy(t, size).start()

        @pl.when((section == 0) & (to == 0))
        def _():
            pbuf[pl.ds(pl.multiple_of(start, fine), size), :] = sbuf[at, :]

    block = 256

    def weight_step(m):
        size = rows * sections
        at = pl.ds(pl.multiple_of(m * size, size), size)

        def column(b, carry):
            cols = pl.ds(pl.multiple_of(b * block, block), block)
            grown = dot(x_v[at, cols], slopes[at, :], TN)
            spot = pl.ds(b * (block // 32), block // 32)
            grown = grown.reshape(block // 32, 2, 16, hidden)

            @pl.when(m == 0)
            def _():
                wacc[spot] = grown

            @pl.when(m > 0)
            def _():
                wacc[spot] = wacc[spot] + grown
            return carry

        lax.fori_loop(0, hidden // block, column, 0)

    sibling = {"owner_2": 1 - pc}
    core_copy = remote(wsend, wrecv, ac_send, ac_recv, sibling)

    def weight_core():
        def cast(k, carry):
            wsend[k] = wacc[k, 1 - pc].astype(BF16)
            return carry

        lax.fori_loop(0, nx * nz, cast, 0)
        core_copy.start()

    def x_send(d):
        to = lax.rem(px + d, nx)
        return remote(part(wx, to, nz), wxr.at[d - 1], bx_send.at[d - 1], bx_recv.at[d - 1],
                      {"owner_0": to})

    def z_send(d):
        to = lax.rem(pz + d, nz)
        return remote(wz.at[to], wzr.at[d - 1], cz_send.at[d - 1], cz_recv.at[d - 1],
                      {"owner_1": to})

    def z_first(d):
        to = lax.rem(pz + d, nz)
        return remote(part(vz, to, nx), vzr.at[d - 1], bz_send.at[d - 1], bz_recv.at[d - 1],
                      {"owner_1": to})

    def x_second(d):
        to = lax.rem(px + d, nx)
        return remote(vx.at[to], vxr.at[d - 1], cx_send.at[d - 1], cx_recv.at[d - 1],
                      {"owner_0": to})

    cut = wx.shape[-1]

    def weight_x():
        core_copy.wait_recv()

        def join(k, carry):
            both = (wacc[k, pc] + wrecv[k].astype(F32)).astype(BF16)
            wx[k] = both[:, :cut]
            vz[lax.rem(k, nz) * nx + k // nz] = both[:, cut:]
            return carry

        lax.fori_loop(0, nx * nz, join, 0)
        for d in range(1, nz):
            z_first(d).start()
        for d in range(1, nx):
            x_send(d).start()

    def weight_z():
        for d in range(1, nx):
            x_send(d).wait_recv()

        def join(k, carry):
            total = wx[px * nz + k].astype(F32)
            for d in range(nx - 1):
                total = total + wxr[d, k].astype(F32)
            wz[k] = total.astype(BF16)
            return carry

        lax.fori_loop(0, nz, join, 0)
        for d in range(1, nz):
            z_send(d).start()
        for d in range(1, nz):
            z_first(d).wait_recv()

        def join_second(k, carry):
            total = vz[pz * nx + k].astype(F32)
            for d in range(nz - 1):
                total = total + vzr[d, k].astype(F32)
            vx[k] = total.astype(BF16)
            return carry

        lax.fori_loop(0, nx, join_second, 0)
        for d in range(1, nx):
            x_second(d).start()

    def weight_end():
        total = wz[pz].astype(F32)
        for d in range(1, nz):
            z_send(d).wait_recv()
            total = total + wzr[d - 1].astype(F32)
        wg_out[:, :cut] = total * scale
        total = vx[px].astype(F32)
        for d in range(1, nx):
            x_second(d).wait_recv()
            total = total + vxr[d - 1].astype(F32)
        wg_out[:, cut:] = total * scale

    def feature_open(i):
        @pl.when(i == 0)
        def _():
            emb_copy.wait()

        @pl.when(section > 0)
        def _():
            here = part(pbuf, i, rows)
            pltpu.make_async_copy(here, here, p_recv.at[i]).wait()

        p = pbuf[pl.ds(pl.multiple_of(i * rows, rows), rows), :]
        s = dot(p, fold[...], NN).astype(BF16)
        blocks = hidden // 128
        tall = jnp.concatenate([s[:, 128 * b:128 * b + 128] for b in range(blocks)], axis=0)
        per = 128 // features
        own_row = lax.rem(lax.broadcasted_iota(jnp.int32, (rows, wide), 0), GROUP)
        own_lane = lax.broadcasted_iota(jnp.int32, (rows, wide), 1) // features
        for j in range(per):
            e = dot(tall, pick[j], NN)
            for b in range(blocks):
                kept = jnp.where(own_row == own_lane, e[rows * b:rows * b + rows], 0.0)
                spread[b * per + j] = kept.astype(BF16)

    def feature_close(i):
        for g in range(rows // GROUP):
            lhs = spread[:, GROUP * g:GROUP * g + GROUP, :].reshape(features * GROUP, wide)
            at = pl.multiple_of((i * (rows // GROUP) + g) * wide, wide)
            out = dot(lhs, emb_v[pl.ds(at, wide), :], NN)
            fg[i, :, GROUP * g:GROUP * g + GROUP, :] = out.astype(BF16).reshape(features, GROUP, lanes)

        core = lax.rem(i, 2)
        def send(step, carry):
            tx, cz, k, own_chip, feature = gather_at(nx * nz - 1 - step)
            arrived = f_recv.at[i // 2, px, jnp.where(k >= near_z, 1, 0)]
            src = fg.at[i, feature]
            slot = pl.ds(pl.multiple_of((k * 2 + pc) * rows, rows), rows)
            dst = arr.at[i // 2, px, slot]
            home = own_chip & (pc == core)

            @pl.when(home)
            def _():
                pltpu.make_async_copy(src, dst, arrived).start()

            @pl.when(jnp.logical_not(home))
            def _():
                remote(src, dst, f_send.at[i], arrived,
                       {"owner_0": tx, "owner_1": cz, "owner_2": core}).start()
            return carry

        lax.fori_loop(0, nx * nz, send, 0)

    table_rows = acc.shape[1]

    def table_part(i, role):
        h = i // 2
        row = lax.broadcasted_iota(jnp.int32, (table_rows, 2 * rows), 0)
        low, high = ((0, near_z), (near_z, nz))[role]
        span = pl.ds(low * 2 * rows, (high - low) * 2 * rows)

        def gather(g, carry):
            landed = arr.at[h, g, span]
            pltpu.make_async_copy(landed, landed, f_recv.at[h, g, role]).wait()
            for z in range(low, high):
                both = idr[(g * nz + z) * 2] + idr[(g * nz + z) * 2 + 1]
                ids = jnp.where(h == 0, both[:, :2 * rows], both[:, 2 * rows:])
                onehot[:, z * 2 * rows:(z + 1) * 2 * rows] = jnp.where(row == ids, 1.0, 0.0).astype(BF16)
            acc[role] = acc[role] + dot(onehot[:, span], arr[h, g, span, :], NN)
            return carry

        lax.fori_loop(0, nx, gather, 0)

    def by_section(*values):
        chosen = values[-1]
        for n in range(sections - 1):
            chosen = jnp.where(section == n, values[n], chosen)
        return chosen

    features_at = (
        (by_section(8, 9, 12, 21), by_section(9, 10, 13, 21)),
        (by_section(10, 13, 16, 26), by_section(12, 14, 17, 26)),
        (by_section(13, 17, 21, 30), by_section(14, 18, 21, 30)),
        (by_section(17, 21, 23, 34), by_section(18, 21, 23, 34)),
    )
    far_table = jnp.where(pc == 0, by_section(15, 22, 22, 31), by_section(21, 22, 22, 35))
    own_table = far_table + by_section(1, 0, 0, 0)
    meet_time = by_section(5, 8, 10, 19)
    x_time = by_section(20, 20, 20, 22)
    z_time = by_section(40, 40, 40, 27)
    ends = 36

    def tick(now, carry):
        for stage in range(3):
            @pl.when((section == 0) & (now == stage))
            def _():
                meet(stage)

        @pl.when(now < small)
        def _():
            chain_step(now, fine)

        @pl.when((now >= small) & (now < chunks))
        def _():
            chain_step(now, rows)

        @pl.when(now == meet_time)
        def _():
            exchange_ids()

        @pl.when(last & (now == 6))
        def _():
            prepare()

        done = now + 1 - small

        @pl.when((now < chunks) & (done >= 0) & (lax.rem(done, sections) == 0))
        def _():
            @pl.when(done == 0)
            def _():
                x_copy.wait()
            weight_step(done // sections)

        @pl.when(now == chunks)
        def _():
            weight_core()

        opened = micros
        closed = micros
        for n in range(micros):
            opened = jnp.where(now == features_at[n][0], n, opened)
            closed = jnp.where(now == features_at[n][1], n, closed)

        @pl.when(opened < micros)
        def _():
            feature_open(opened)

        @pl.when(closed < micros)
        def _():
            feature_close(closed)

        @pl.when(now == far_table)
        def _():
            pltpu.make_async_copy(idr, idr, id_recv).wait()
            table_part(pc, 1)

        @pl.when(now == own_table)
        def _():
            table_part(pc, 0)

        @pl.when(now == x_time)
        def _():
            weight_x()

        @pl.when(now == z_time)
        def _():
            weight_z()
        return carry

    lax.fori_loop(0, ends, tick, 0)

    half = table_rows // 2
    piece = half // sections

    def sib_copy(q):
        return remote(part(acc.at[q], 1 - pc, half), sib.at[q], sib_send.at[q], sib_recv.at[q], sibling)

    def y_copy(d, q):
        to = lax.rem(section + d, sections)
        return remote(part(ysend.at[q], to, piece), yrecv.at[d - 1, q],
                      y_send.at[d - 1, q], y_recv.at[d - 1, q], {"section": to})

    def settle(q):
        sib_copy(q).wait()
        mine = pl.ds(pl.multiple_of(pc * half, half), half)
        sib[q] = sib[q] + acc[q, mine, :]
        ysend[q] = sib[q].astype(BF16)
        for d in range(1, sections):
            y_copy(d, q).start()

    table_part(2 + pc, 1)
    sib_copy(1).start()
    table_part(2 + pc, 0)
    sib_copy(0).start()

    @pl.when(z_time > ends)
    def _():
        weight_z()

    settle(1)
    settle(0)

    def gathered(q):
        total = part(sib.at[q], section, piece)[...]
        for d in range(1, sections):
            y_copy(d, q).wait_recv()
            total = total + yrecv[d - 1, q].astype(F32)
        return total

    far_copy = remote(fsend, frecv, far_send, far_recv, {"owner_1": lax.rem(pz + nz // 2, nz)})
    fsend[...] = gathered(1).astype(BF16)
    far_copy.start()
    total = gathered(0)
    weight_end()
    far_copy.wait_recv()
    tg_out[...] = (total + frecv[...].astype(F32)) * scale

    def finish(t, size):
        @pl.when(section > 0)
        def _():
            down_copy(t, size).wait_send()

        @pl.when((section == 0) & (p_place(t, size)[0] > 0))
        def _():
            p_copy(t, size).wait_send()

    each_chunk(finish)
    some = pl.ds(0, 2 * nx * nz - 2)
    pltpu.make_async_copy(ids_v.at[some], ids_v.at[some], id_send).wait()
    for i in range(micros):
        @pl.when(pc == i % 2)
        def _():
            sent = fg.at[i, pl.ds(0, features - 2)]
            pltpu.make_async_copy(sent, sent, f_send.at[i]).wait()

        @pl.when(pc != i % 2)
        def _():
            sent = fg.at[i]
            pltpu.make_async_copy(sent, sent, f_send.at[i]).wait()
    core_copy.wait_send()
    for d in range(1, nx):
        x_send(d).wait_send()
        x_second(d).wait_send()
    for d in range(1, nz):
        z_send(d).wait_send()
        z_first(d).wait_send()
    for q in range(2):
        for d in range(1, sections):
            y_copy(d, q).wait_send()
    far_copy.wait_send()


def hand_on(a_ref, b_ref, a_out, b_out):
    a_out[...] = a_ref[...]
    b_out[...] = b_ref[...]


def per_device(weights, inputs, preact, cotangent, embeddings, row_ids):
    sections = lax.axis_size("section")
    nx, nz, cores = (lax.axis_size(a) for a in OWNER)
    micros, batch_rows, hidden = cotangent.shape
    quarter, features, width = embeddings.shape[1:]
    total = micros * batch_rows
    owners = nx * nz * cores
    scale = 1.0 / math.sqrt(total * owners)
    table_rows = 1024
    ids_shape = (owners, 1, 2 * cores * quarter)
    dma = pltpu.SemaphoreType.DMA
    vmem = pl.BlockSpec(memory_space=pltpu.VMEM)
    hbm = pl.BlockSpec(memory_space=pl.ANY)
    chunks = (micros + 1) * sections
    rows = total // (micros * sections)
    wide = GROUP * features
    part = hidden // owners
    half = table_rows // 2
    cut = hidden * 3 // 4
    V = pltpu.VMEM
    weight_grad, table_grad = pl.pallas_call(
        functools.partial(step_kernel, (micros, sections, nx, nz, features), scale),
        out_shape=(
            jax.ShapeDtypeStruct((part, hidden), F32),
            jax.ShapeDtypeStruct((half // sections, width), F32),
        ),
        in_specs=[hbm] * 6,
        out_specs=(vmem, vmem),
        scratch_shapes=[
            V((hidden, hidden), BF16),
            V((hidden, hidden), BF16),
            V((total, hidden), BF16),
            V((total, hidden), BF16),
            V((micros * quarter * features, width), BF16),
            V((micros, features, quarter), jnp.int32),
            V(ids_shape, jnp.int32),
            V((total, hidden), BF16),
            V((total, hidden), BF16),
            V((total, hidden), BF16),
            V((micros * quarter, hidden), BF16),
            V((nx * nz, 2, part, hidden), F32),
            V((nx * nz, part, hidden), BF16),
            V((nx * nz, part, hidden), BF16),
            V((nx * nz, part, cut), BF16),
            V((nx - 1, nz, part, cut), BF16),
            V((nz, part, cut), BF16),
            V((nz - 1, part, cut), BF16),
            V((nx * nz, part, hidden - cut), BF16),
            V((nz - 1, nx, part, hidden - cut), BF16),
            V((nx, part, hidden - cut), BF16),
            V((nx - 1, part, hidden - cut), BF16),
            V((hidden, hidden), BF16),
            V((128 // features, 128, wide), BF16),
            V((features, rows, wide), BF16),
            V((micros, features, rows, width), BF16),
            V((micros // 2, nx, nz * 2 * rows, width), BF16),
            V(ids_shape, jnp.int32),
            V((table_rows, nz * 2 * rows), BF16),
            V((2, table_rows, width), F32),
            V((2, half, width), F32),
            V((2, half, width), BF16),
            V((sections - 1, 2, half // sections, width), BF16),
            V((half // sections, width), BF16),
            V((half // sections, width), BF16),
            pltpu.SemaphoreType.REGULAR((4,)),
            dma, dma, dma((chunks,)), dma, dma, dma((chunks,)), dma((chunks,)),
            dma((micros,)), dma((chunks,)),
            dma, dma, dma((micros,)), dma((micros // 2, nx, 2)),
            dma, dma, dma((nx - 1,)), dma((nx - 1,)), dma((nz - 1,)), dma((nz - 1,)),
            dma((nz - 1,)), dma((nz - 1,)), dma((nx - 1,)), dma((nx - 1,)),
            dma((2,)), dma((2,)), dma((sections - 1, 2)), dma((sections - 1, 2)), dma, dma,
        ],
        compiler_params=pltpu.CompilerParams(
            collective_id=0, has_side_effects=True, vmem_limit_bytes=60 * 1024 * 1024
        ),
    )(
        weights[0],
        inputs.reshape(total, hidden),
        preact.reshape(total, hidden),
        cotangent.reshape(total, hidden),
        embeddings.reshape(micros * quarter * features, width),
        row_ids.transpose(0, 2, 1),
    )
    weight_grad, table_grad = pl.pallas_call(
        hand_on,
        out_shape=(
            jax.ShapeDtypeStruct(weight_grad.shape, F32),
            jax.ShapeDtypeStruct(table_grad.shape, F32),
        ),
        in_specs=[vmem] * 2,
        out_specs=(vmem, vmem),
    )(weight_grad, table_grad)
    return (weight_grad[None], table_grad[None])


def solution(mesh):
    finer = Mesh(
        mesh.devices.reshape(mesh.shape["section"], 4, 8, 2),
        ("section", "owner_0", "owner_1", "owner_2"),
    )
    placed = (
        P("section", None, None),
        P("section", None, OWNER, None),
        P("section", None, OWNER, None),
        P(None, OWNER, None),
        P(None, OWNER_SECTION, None, None),
        P(None, OWNER_SECTION, None),
    )
    return jax.shard_map(
        per_device,
        mesh=finer,
        in_specs=placed,
        out_specs=(P("section", OWNER, None), P(OWNER, "section", None)),
        check_vma=False,
    )
```

```python
import functools
import math

import jax
import jax.numpy as jnp
from jax import lax
from jax.experimental import pallas as pl
from jax.experimental.pallas import tpu as pltpu
from jax.sharding import Mesh
from jax.sharding import PartitionSpec as P

OWNER = ("owner_0", "owner_1", "owner_2")
OWNER_SECTION = ("owner_0", "owner_1", "owner_2", "section")
MESH = pl.DeviceIdType.MESH
BF16 = jnp.bfloat16
F32 = jnp.float32
NN = (((1,), (0,)), ((), ()))
NT = (((1,), (1,)), ((), ()))
TN = (((0,), (0,)), ((), ()))
GROUP = 16


def dot(a, b, dims):
    return lax.dot_general(a, b, dims, preferred_element_type=F32)


def step_kernel(
    dims, scale,
    w_hbm, x_hbm, pre_hbm, cot_hbm, emb_hbm, ids_hbm,
    wg_out, tg_out,
    w_v, wt_v, x_v, pre_v, emb_v, raw_v, ids_v, rbuf, sbuf, slopes, pbuf, wacc, wsend, wrecv, wx, wxr, wz, wzr, vz, vzr, vx, vxr,
    fold, pick, spread, fg, arr, idr, onehot, acc, sib, ysend, yrecv, fsend, frecv,
    near, w_sem, x_sem, pre_sem, emb_sem, ids_sem, in_sem, out_sem, p_recv, p_send,
    id_send, id_recv, f_send, f_recv, ac_send, ac_recv, bx_send, bx_recv, cz_send, cz_recv, bz_send, bz_recv, cx_send, cx_recv,
    sib_send, sib_recv, y_send, y_recv, far_send, far_recv,
):
    micros, sections, nx, nz, features = dims
    section = lax.axis_index("section")
    px = lax.axis_index("owner_0")
    pz = lax.axis_index("owner_1")
    pc = lax.axis_index("owner_2")
    rows = pre_v.shape[0] // (micros * sections)
    fine = rows // 2
    group = 2 * sections
    chunks = group * micros
    hidden = w_v.shape[0]
    lanes = emb_v.shape[1]
    last = section == sections - 1

    def part(ref, t, size):
        return ref.at[pl.ds(pl.multiple_of(t * size, size), size)]

    def spot(t):
        return pl.ds(pl.multiple_of(t * fine, fine), fine)

    def each_chunk(body):
        def one(t, carry):
            body(t)
            return carry

        lax.fori_loop(0, chunks, one, 0)

    def pre_copy(t):
        return pltpu.make_async_copy(pre_hbm.at[spot(t)], pre_v.at[spot(t)], pre_sem.at[t])

    def cot_copy(t):
        return pltpu.make_async_copy(cot_hbm.at[spot(t)], rbuf.at[spot(t)], in_sem.at[t])

    def remote(src, dst, send, recv, where):
        return pltpu.make_async_remote_copy(
            src_ref=src, dst_ref=dst, send_sem=send, recv_sem=recv,
            device_id=where, device_id_type=MESH,
        )

    def down_copy(t):
        return remote(
            sbuf.at[spot(t)], rbuf.at[spot(t)], out_sem.at[t], in_sem.at[t],
            {"section": lax.rem(section + sections - 1, sections)},
        )

    def p_place(t):
        unit = t // group
        start = unit * rows + lax.rem(t, 2) * fine
        return lax.rem(t, group) // 2, unit, pl.ds(pl.multiple_of(start, fine), fine)

    def p_copy(t):
        to, unit, at = p_place(t)
        return remote(
            sbuf.at[spot(t)], pbuf.at[at], p_send.at[t], p_recv.at[unit], {"section": to}
        )

    def chip(n):
        dx = lax.rem(n, nx)
        k = n // nx
        dz = ((k + 1) // 2) * (2 * lax.rem(k, 2) - 1)
        return lax.rem(px + dx, nx), lax.rem(pz + dz + nz, nz)

    w_copy = pltpu.make_async_copy(w_hbm, w_v, w_sem)
    x_copy = pltpu.make_async_copy(x_hbm, x_v, x_sem)
    emb_copy = pltpu.make_async_copy(emb_hbm, emb_v, emb_sem)
    ids_copy = pltpu.make_async_copy(ids_hbm, raw_v, ids_sem)
    barrier = pltpu.get_barrier_semaphore()

    def peers(name, place, count, sem):
        for d in range(1, count):
            pl.semaphore_signal(
                sem, inc=1, device_id={name: lax.rem(place + d, count)}, device_id_type=MESH
            )

    inner = (("owner_1", pz, nz), ("owner_0", px, nx), ("owner_2", pc, 2))
    peers("section", section, sections, barrier)

    @pl.when(section == 0)
    def _():
        for name, place, count in inner:
            peers(name, place, count, barrier)

    w_copy.start()

    def begin(t):
        pre_copy(t).start()

        @pl.when(last)
        def _():
            cot_copy(t).start()

    each_chunk(begin)
    ids_copy.start()
    emb_copy.start()
    x_copy.start()

    @pl.when(section == 0)
    def _():
        pl.semaphore_wait(barrier, sections - 1 + sum(count - 1 for name, place, count in inner))

    @pl.when(section > 0)
    def _():
        pl.semaphore_wait(barrier, sections - 1)

    wide = GROUP * features

    def prepare():
        across = lax.broadcasted_iota(jnp.int32, (128, hidden), 1)
        flipped = lax.rem(across, features) * features + across // features

        def make_fold(b, carry):
            down = lax.broadcasted_iota(jnp.int32, (128, hidden), 0) + b * 128
            value = jnp.where(down == across, 1.0, 0.0) + jnp.where(down == flipped, 1.0, 0.0)
            part(fold, b, 128)[...] = value.astype(BF16)
            return carry

        lax.fori_loop(0, hidden // 128, make_fold, 0)
        for j in range(128 // features):
            down = lax.broadcasted_iota(jnp.int32, (128, wide), 0)
            col = lax.rem(lax.broadcasted_iota(jnp.int32, (128, wide), 1), features) + j * features
            pick[j] = jnp.where(down == col, 1.0, 0.0).astype(BF16)
        acc[...] = jnp.zeros_like(acc)
        ids_copy.wait()
        owner_lane = lax.rem(lax.broadcasted_iota(jnp.int32, (features, 4 * rows), 1) // rows, 2)
        for r in range(2):
            first, second = raw_v[r], raw_v[2 + r]
            spaced = jnp.concatenate([first, first, second, second], axis=1)
            spaced = jnp.where(owner_lane == pc, spaced, 0)
            for f in range(features):
                ids_v[f * 2 + r] = spaced[f:f + 1, :]

    near_z = nz // 2 + 1

    def gather_at(n):
        tx, tz = chip(n)
        k = n // nx
        far = k >= near_z
        home = (lax.rem(n, nx) == 0) & ((k == 0) | (k == nz - 1))
        return tx, lax.rem(tz + jnp.where(far, nz // 2, 0), nz), k, home, tx * nz + tz

    def send_ids(n, carry):
        tx, cz, k, own_chip, feature = gather_at(n)
        mine = (px * nz + k) * 2 + pc
        for r in range(2):
            there = feature * 2 + r
            home = own_chip & (pc == r)

            @pl.when(home)
            def _():
                pltpu.make_async_copy(ids_v.at[there], idr.at[mine], id_recv).start()

            @pl.when(jnp.logical_not(home))
            def _():
                remote(
                    ids_v.at[there], idr.at[mine], id_send, id_recv,
                    {"owner_0": tx, "owner_1": cz, "owner_2": r},
                ).start()
        return carry

    @pl.when(section == 0)
    def _():
        peers(*inner[0], near.at[0])

    def meet(stage):
        pl.semaphore_wait(near.at[stage], inner[stage][2] - 1)
        if stage < 2:
            peers(*inner[stage + 1], near.at[stage + 1])
        else:
            peers("section", section, sections, near.at[3])

    def exchange_ids():
        @pl.when(section > 0)
        def _():
            pl.semaphore_wait(near.at[3], 1)

        lax.fori_loop(0, nx * nz, send_ids, 0)

    w_copy.wait()

    @pl.when(jnp.logical_not(last))
    def _():
        def turn(b, carry):
            cols = pl.ds(pl.multiple_of(b * 128, 128), 128)
            wt_v[:, cols] = part(w_v, b, 128)[...].T
            return carry

        lax.fori_loop(0, hidden // 128, turn, 0)
        prepare()

    def chain_step(t):
        pre_copy(t).wait()

        @pl.when(last)
        def _():
            cot_copy(t).wait()

        @pl.when(jnp.logical_not(last))
        def _():
            down_copy(t).wait_recv()

        at = spot(t)
        incoming = rbuf[at, :]
        slope = jnp.where(pre_v[at, :] > 0, incoming, jnp.zeros_like(incoming))
        slopes[at, :] = slope

        @pl.when(last)
        def _():
            sbuf[at, :] = dot(slope, w_v[...], NT).astype(BF16)

        @pl.when(jnp.logical_not(last))
        def _():
            sbuf[at, :] = dot(slope, wt_v[...], NN).astype(BF16)

        @pl.when(section > 0)
        def _():
            down_copy(t).start()

        to, unit, place = p_place(t)

        @pl.when((section == 0) & (to > 0))
        def _():
            p_copy(t).start()

        @pl.when((section == 0) & (to == 0))
        def _():
            pbuf[place, :] = sbuf[at, :]

    block = 256

    def weight_step(m):
        size = rows * sections
        at = pl.ds(pl.multiple_of(m * size, size), size)

        def column(b, carry):
            cols = pl.ds(pl.multiple_of(b * block, block), block)
            grown = dot(x_v[at, cols], slopes[at, :], TN)
            spot = pl.ds(b * (block // 32), block // 32)
            grown = grown.reshape(block // 32, 2, 16, hidden)

            @pl.when(m == 0)
            def _():
                wacc[spot] = grown

            @pl.when(m > 0)
            def _():
                wacc[spot] = wacc[spot] + grown
            return carry

        lax.fori_loop(0, hidden // block, column, 0)

    sibling = {"owner_2": 1 - pc}
    core_copy = remote(wsend, wrecv, ac_send, ac_recv, sibling)

    def weight_core():
        def cast(k, carry):
            wsend[k] = wacc[k, 1 - pc].astype(BF16)
            return carry

        lax.fori_loop(0, nx * nz, cast, 0)
        core_copy.start()

    def x_send(d):
        to = lax.rem(px + d, nx)
        return remote(part(wx, to, nz), wxr.at[d - 1], bx_send.at[d - 1], bx_recv.at[d - 1],
                      {"owner_0": to})

    def z_send(d):
        to = lax.rem(pz + d, nz)
        return remote(wz.at[to], wzr.at[d - 1], cz_send.at[d - 1], cz_recv.at[d - 1],
                      {"owner_1": to})

    def z_first(d):
        to = lax.rem(pz + d, nz)
        return remote(part(vz, to, nx), vzr.at[d - 1], bz_send.at[d - 1], bz_recv.at[d - 1],
                      {"owner_1": to})

    def x_second(d):
        to = lax.rem(px + d, nx)
        return remote(vx.at[to], vxr.at[d - 1], cx_send.at[d - 1], cx_recv.at[d - 1],
                      {"owner_0": to})

    cut = wx.shape[-1]

    def weight_x():
        core_copy.wait_recv()

        def join(k, carry):
            both = (wacc[k, pc] + wrecv[k].astype(F32)).astype(BF16)
            wx[k] = both[:, :cut]
            vz[lax.rem(k, nz) * nx + k // nz] = both[:, cut:]
            return carry

        lax.fori_loop(0, nx * nz, join, 0)
        for d in range(1, nz):
            z_first(d).start()
        for d in range(1, nx):
            x_send(d).start()

    def weight_z():
        for d in range(1, nx):
            x_send(d).wait_recv()

        def join(k, carry):
            total = wx[px * nz + k].astype(F32)
            for d in range(nx - 1):
                total = total + wxr[d, k].astype(F32)
            wz[k] = total.astype(BF16)
            return carry

        lax.fori_loop(0, nz, join, 0)
        for d in range(1, nz):
            z_send(d).start()
        for d in range(1, nz):
            z_first(d).wait_recv()

        def join_second(k, carry):
            total = vz[pz * nx + k].astype(F32)
            for d in range(nz - 1):
                total = total + vzr[d, k].astype(F32)
            vx[k] = total.astype(BF16)
            return carry

        lax.fori_loop(0, nx, join_second, 0)
        for d in range(1, nx):
            x_second(d).start()

    def weight_end():
        total = wz[pz].astype(F32)
        for d in range(1, nz):
            z_send(d).wait_recv()
            total = total + wzr[d - 1].astype(F32)
        wg_out[:, :cut] = total * scale
        total = vx[px].astype(F32)
        for d in range(1, nx):
            x_second(d).wait_recv()
            total = total + vxr[d - 1].astype(F32)
        wg_out[:, cut:] = total * scale

    def feature_open(i):
        @pl.when(i == 0)
        def _():
            emb_copy.wait()

        @pl.when(section > 0)
        def _():
            here = part(pbuf, i, rows)
            pltpu.make_async_copy(here, here, p_recv.at[i]).wait()

        p = pbuf[pl.ds(pl.multiple_of(i * rows, rows), rows), :]
        s = dot(p, fold[...], NN).astype(BF16)
        blocks = hidden // 128
        tall = jnp.concatenate([s[:, 128 * b:128 * b + 128] for b in range(blocks)], axis=0)
        per = 128 // features
        own_row = lax.rem(lax.broadcasted_iota(jnp.int32, (rows, wide), 0), GROUP)
        own_lane = lax.broadcasted_iota(jnp.int32, (rows, wide), 1) // features
        for j in range(per):
            e = dot(tall, pick[j], NN)
            for b in range(blocks):
                kept = jnp.where(own_row == own_lane, e[rows * b:rows * b + rows], 0.0)
                spread[b * per + j] = kept.astype(BF16)

    def feature_close(i):
        for g in range(rows // GROUP):
            lhs = spread[:, GROUP * g:GROUP * g + GROUP, :].reshape(features * GROUP, wide)
            at = pl.multiple_of((i * (rows // GROUP) + g) * wide, wide)
            out = dot(lhs, emb_v[pl.ds(at, wide), :], NN)
            fg[i, :, GROUP * g:GROUP * g + GROUP, :] = out.astype(BF16).reshape(features, GROUP, lanes)

        core = lax.rem(i, 2)
        def send(step):
            tx, cz, k, own_chip, feature = gather_at(nx * nz - 1 - step)
            arrived = f_recv.at[i // 2, px, jnp.where(k >= near_z, 1, 0)]
            src = fg.at[i, feature]
            slot = pl.ds(pl.multiple_of((k * 2 + pc) * rows, rows), rows)
            dst = arr.at[i // 2, px, slot]
            home = own_chip & (pc == core)

            @pl.when(home)
            def _():
                pltpu.make_async_copy(src, dst, arrived).start()

            @pl.when(jnp.logical_not(home))
            def _():
                remote(src, dst, f_send.at[i], arrived,
                       {"owner_0": tx, "owner_1": cz, "owner_2": core}).start()

        for step in range(nx * nz):
            send(step)

    table_rows = acc.shape[1]

    def mark_rows(i):
        row = lax.broadcasted_iota(jnp.int32, (table_rows, 2 * rows), 0)

        def mark(g, carry):
            for z in range(nz):
                both = idr[(g * nz + z) * 2] + idr[(g * nz + z) * 2 + 1]
                ids = jnp.where(i < 2, both[:, :2 * rows], both[:, 2 * rows:])
                onehot[g, :, z * 2 * rows:(z + 1) * 2 * rows] = jnp.where(row == ids, 1.0, 0.0).astype(BF16)
            return carry

        lax.fori_loop(0, nx, mark, 0)

    def table_part(i, role):
        h = i // 2
        low, high = ((0, near_z), (near_z, nz))[role]
        span = pl.ds(low * 2 * rows, (high - low) * 2 * rows)

        def gather(g, carry):
            landed = arr.at[h, g, span]
            pltpu.make_async_copy(landed, landed, f_recv.at[h, g, role]).wait()
            acc[role] = acc[role] + dot(onehot[g, :, span], arr[h, g, span, :], NN)
            return carry

        lax.fori_loop(0, nx, gather, 0)

    def by_section(*values):
        chosen = values[-1]
        for n in range(sections - 1):
            chosen = jnp.where(section == n, values[n], chosen)
        return chosen

    features_at = (
        (by_section(8, 11, 17, 22), by_section(10, 13, 18, 22)),
        (by_section(12, 20, 26, 38), by_section(14, 22, 27, 38)),
        (by_section(18, 28, 33, 42), by_section(20, 30, 33, 42)),
        (by_section(26, 33, 35, 46), by_section(28, 33, 35, 46)),
    )
    table_at = jnp.where(pc == 0, by_section(34, 34, 34, 43), by_section(34, 34, 34, 47))
    meet_time = by_section(5, 8, 12, 20)
    x_time = by_section(33, 33, 36, 46)
    ends = 48

    def tick(now, carry):
        for stage in range(3):
            @pl.when((section == 0) & (now == stage))
            def _():
                meet(stage)

        @pl.when(now < chunks)
        def _():
            chain_step(now)

        @pl.when(now == meet_time)
        def _():
            exchange_ids()

        @pl.when(last & (now == 6))
        def _():
            prepare()

        done = now + 1

        @pl.when((now < chunks) & (lax.rem(done, group) == 0))
        def _():
            @pl.when(done == group)
            def _():
                x_copy.wait()
            weight_step(done // group - 1)

        @pl.when(now == chunks)
        def _():
            weight_core()

        opened = micros
        closed = micros
        for n in range(micros):
            opened = jnp.where(now == features_at[n][0], n, opened)
            closed = jnp.where(now == features_at[n][1], n, closed)

        @pl.when(opened < micros)
        def _():
            feature_open(opened)

        @pl.when(closed < micros)
        def _():
            feature_close(closed)

        @pl.when(now == table_at)
        def _():
            pltpu.make_async_copy(idr, idr, id_recv).wait()
            mark_rows(pc)
            table_part(pc, 1)
            table_part(pc, 0)

        @pl.when(now == x_time)
        def _():
            weight_x()

        return carry

    lax.fori_loop(0, ends, tick, 0)

    half = table_rows // 2
    piece = half // sections

    def sib_copy(q):
        return remote(part(acc.at[q], 1 - pc, half), sib.at[q], sib_send.at[q], sib_recv.at[q], sibling)

    def y_copy(d, q):
        to = lax.rem(section + d, sections)
        return remote(part(ysend.at[q], to, piece), yrecv.at[d - 1, q],
                      y_send.at[d - 1, q], y_recv.at[d - 1, q], {"section": to})

    def settle(q):
        sib_copy(q).wait()
        mine = pl.ds(pl.multiple_of(pc * half, half), half)
        sib[q] = sib[q] + acc[q, mine, :]
        ysend[q] = sib[q].astype(BF16)
        for d in range(1, sections):
            y_copy(d, q).start()

    mark_rows(2 + pc)
    table_part(2 + pc, 1)
    sib_copy(1).start()
    table_part(2 + pc, 0)
    sib_copy(0).start()

    weight_z()

    settle(1)
    settle(0)

    def gathered(q):
        total = part(sib.at[q], section, piece)[...]
        for d in range(1, sections):
            y_copy(d, q).wait_recv()
            total = total + yrecv[d - 1, q].astype(F32)
        return total

    far_copy = remote(fsend, frecv, far_send, far_recv, {"owner_1": lax.rem(pz + nz // 2, nz)})
    fsend[...] = gathered(1).astype(BF16)
    far_copy.start()
    total = gathered(0)
    weight_end()
    far_copy.wait_recv()
    tg_out[...] = (total + frecv[...].astype(F32)) * scale

    def finish(t):
        @pl.when(section > 0)
        def _():
            down_copy(t).wait_send()

        @pl.when((section == 0) & (p_place(t)[0] > 0))
        def _():
            p_copy(t).wait_send()

    each_chunk(finish)
    some = pl.ds(0, 2 * nx * nz - 2)
    pltpu.make_async_copy(ids_v.at[some], ids_v.at[some], id_send).wait()
    for i in range(micros):
        @pl.when(pc == i % 2)
        def _():
            sent = fg.at[i, pl.ds(0, features - 2)]
            pltpu.make_async_copy(sent, sent, f_send.at[i]).wait()

        @pl.when(pc != i % 2)
        def _():
            sent = fg.at[i]
            pltpu.make_async_copy(sent, sent, f_send.at[i]).wait()
    core_copy.wait_send()
    for d in range(1, nx):
        x_send(d).wait_send()
        x_second(d).wait_send()
    for d in range(1, nz):
        z_send(d).wait_send()
        z_first(d).wait_send()
    for q in range(2):
        for d in range(1, sections):
            y_copy(d, q).wait_send()
    far_copy.wait_send()


def hand_on(a_ref, b_ref, a_out, b_out):
    a_out[...] = a_ref[...]
    b_out[...] = b_ref[...]


def per_device(weights, inputs, preact, cotangent, embeddings, row_ids):
    sections = lax.axis_size("section")
    nx, nz, cores = (lax.axis_size(a) for a in OWNER)
    micros, batch_rows, hidden = cotangent.shape
    quarter, features, width = embeddings.shape[1:]
    total = micros * batch_rows
    owners = nx * nz * cores
    scale = 1.0 / math.sqrt(total * owners)
    table_rows = 1024
    ids_shape = (owners, 1, 2 * cores * quarter)
    dma = pltpu.SemaphoreType.DMA
    vmem = pl.BlockSpec(memory_space=pltpu.VMEM)
    hbm = pl.BlockSpec(memory_space=pl.ANY)
    chunks = 2 * sections * micros
    rows = total // (micros * sections)
    wide = GROUP * features
    part = hidden // owners
    half = table_rows // 2
    cut = hidden * 3 // 4
    V = pltpu.VMEM
    weight_grad, table_grad = pl.pallas_call(
        functools.partial(step_kernel, (micros, sections, nx, nz, features), scale),
        out_shape=(V((part, hidden), F32), V((half // sections, width), F32)),
        in_specs=[hbm] * 6,
        out_specs=(vmem, vmem),
        scratch_shapes=[
            V((hidden, hidden), BF16),
            V((hidden, hidden), BF16),
            V((total, hidden), BF16),
            V((total, hidden), BF16),
            V((micros * quarter * features, width), BF16),
            V((micros, features, quarter), jnp.int32),
            V(ids_shape, jnp.int32),
            V((total, hidden), BF16),
            V((total, hidden), BF16),
            V((total, hidden), BF16),
            V((micros * quarter, hidden), BF16),
            V((nx * nz, 2, part, hidden), F32),
            V((nx * nz, part, hidden), BF16),
            V((nx * nz, part, hidden), BF16),
            V((nx * nz, part, cut), BF16),
            V((nx - 1, nz, part, cut), BF16),
            V((nz, part, cut), BF16),
            V((nz - 1, part, cut), BF16),
            V((nx * nz, part, hidden - cut), BF16),
            V((nz - 1, nx, part, hidden - cut), BF16),
            V((nx, part, hidden - cut), BF16),
            V((nx - 1, part, hidden - cut), BF16),
            V((hidden, hidden), BF16),
            V((128 // features, 128, wide), BF16),
            V((features, rows, wide), BF16),
            V((micros, features, rows, width), BF16),
            V((micros // 2, nx, nz * 2 * rows, width), BF16),
            V(ids_shape, jnp.int32),
            V((nx, table_rows, nz * 2 * rows), BF16),
            V((2, table_rows, width), F32),
            V((2, half, width), F32),
            V((2, half, width), BF16),
            V((sections - 1, 2, half // sections, width), BF16),
            V((half // sections, width), BF16),
            V((half // sections, width), BF16),
            pltpu.SemaphoreType.REGULAR((4,)),
            dma, dma, dma((chunks,)), dma, dma, dma((chunks,)), dma((chunks,)),
            dma((micros,)), dma((chunks,)),
            dma, dma, dma((micros,)), dma((micros // 2, nx, 2)),
            dma, dma, dma((nx - 1,)), dma((nx - 1,)), dma((nz - 1,)), dma((nz - 1,)),
            dma((nz - 1,)), dma((nz - 1,)), dma((nx - 1,)), dma((nx - 1,)),
            dma((2,)), dma((2,)), dma((sections - 1, 2)), dma((sections - 1, 2)), dma, dma,
        ],
        compiler_params=pltpu.CompilerParams(
            collective_id=0, has_side_effects=True, vmem_limit_bytes=60 * 1024 * 1024
        ),
    )(
        weights[0],
        inputs.reshape(total, hidden),
        preact.reshape(total, hidden),
        cotangent.reshape(total, hidden),
        embeddings.reshape(micros * quarter * features, width),
        row_ids.transpose(0, 2, 1),
    )
    weight_grad, table_grad = pl.pallas_call(
        hand_on,
        out_shape=(
            jax.ShapeDtypeStruct(weight_grad.shape, F32),
            jax.ShapeDtypeStruct(table_grad.shape, F32),
        ),
        in_specs=[vmem] * 2,
        out_specs=(vmem, vmem),
    )(pltpu.with_memory_space_constraint(weight_grad, pltpu.VMEM), pltpu.with_memory_space_constraint(table_grad, pltpu.VMEM))
    return (weight_grad[None], table_grad[None])


def solution(mesh):
    finer = Mesh(
        mesh.devices.reshape(mesh.shape["section"], 4, 8, 2),
        ("section", "owner_0", "owner_1", "owner_2"),
    )
    placed = (
        P("section", None, None),
        P("section", None, OWNER, None),
        P("section", None, OWNER, None),
        P(None, OWNER, None),
        P(None, OWNER_SECTION, None, None),
        P(None, OWNER_SECTION, None),
    )
    return jax.shard_map(
        per_device,
        mesh=finer,
        in_specs=placed,
        out_specs=(P("section", OWNER, None), P(OWNER, "section", None)),
        check_vma=False,
    )
```

```python
import functools
import math

import jax
import jax.numpy as jnp
from jax import lax
from jax.experimental import pallas as pl
from jax.experimental.pallas import tpu as pltpu
from jax.sharding import Mesh
from jax.sharding import PartitionSpec as P

OWNER = ("owner_0", "owner_1", "owner_2")
OWNER_SECTION = ("owner_0", "owner_1", "owner_2", "section")
MESH = pl.DeviceIdType.MESH
BF16 = jnp.bfloat16
F32 = jnp.float32
NN = (((1,), (0,)), ((), ()))
NT = (((1,), (1,)), ((), ()))
TN = (((0,), (0,)), ((), ()))
GROUP = 16


def dot(a, b, dims):
    return lax.dot_general(a, b, dims, preferred_element_type=F32)


def step_kernel(
    dims, scale,
    w_hbm, x_hbm, pre_hbm, cot_hbm, emb_hbm, ids_hbm,
    wg_out, tg_out,
    w_v, wt_v, x_v, pre_v, emb_v, raw_v, ids_v, rbuf, sbuf, slopes, pbuf, wacc, wsend, wrecv, wx, wxr, wz, wzr, vz, vzr, vx, vxr,
    fold, pick, spread, fg, arr, idr, onehot, acc, sib, ysend, yrecv, fsend, frecv,
    near, w_sem, x_sem, pre_sem, emb_sem, ids_sem, in_sem, out_sem, p_recv, p_send,
    id_send, id_recv, f_send, f_recv, ac_send, ac_recv, bx_send, bx_recv, cz_send, cz_recv, bz_send, bz_recv, cx_send, cx_recv,
    sib_send, sib_recv, y_send, y_recv, far_send, far_recv,
):
    micros, sections, nx, nz, features = dims
    section = lax.axis_index("section")
    px = lax.axis_index("owner_0")
    pz = lax.axis_index("owner_1")
    pc = lax.axis_index("owner_2")
    rows = pre_v.shape[0] // (micros * sections)
    fine = rows // 2
    group = 2 * sections
    chunks = group * micros
    hidden = w_v.shape[0]
    lanes = emb_v.shape[1]
    last = section == sections - 1

    def part(ref, t, size):
        return ref.at[pl.ds(pl.multiple_of(t * size, size), size)]

    def spot(t):
        return pl.ds(pl.multiple_of(t * fine, fine), fine)

    def each_chunk(body):
        def one(t, carry):
            body(t)
            return carry

        lax.fori_loop(0, chunks, one, 0)

    def pre_copy(t):
        return pltpu.make_async_copy(pre_hbm.at[spot(t)], pre_v.at[spot(t)], pre_sem.at[t])

    def cot_copy(t):
        return pltpu.make_async_copy(cot_hbm.at[spot(t)], rbuf.at[spot(t)], in_sem.at[t])

    def remote(src, dst, send, recv, where):
        return pltpu.make_async_remote_copy(
            src_ref=src, dst_ref=dst, send_sem=send, recv_sem=recv,
            device_id=where, device_id_type=MESH,
        )

    def down_copy(t):
        return remote(
            sbuf.at[spot(t)], rbuf.at[spot(t)], out_sem.at[t], in_sem.at[t],
            {"section": lax.rem(section + sections - 1, sections)},
        )

    def p_place(t):
        unit = t // group
        start = unit * rows + lax.rem(t, 2) * fine
        return lax.rem(t, group) // 2, unit, pl.ds(pl.multiple_of(start, fine), fine)

    def p_copy(t):
        to, unit, at = p_place(t)
        return remote(
            sbuf.at[spot(t)], pbuf.at[at], p_send.at[t], p_recv.at[unit], {"section": to}
        )

    def chip(n):
        dx = lax.rem(n, nx)
        k = n // nx
        dz = ((k + 1) // 2) * (2 * lax.rem(k, 2) - 1)
        return lax.rem(px + dx, nx), lax.rem(pz + dz + nz, nz)

    w_copy = pltpu.make_async_copy(w_hbm, w_v, w_sem)
    x_copy = pltpu.make_async_copy(x_hbm, x_v, x_sem)
    emb_copy = pltpu.make_async_copy(emb_hbm, emb_v, emb_sem)
    ids_copy = pltpu.make_async_copy(ids_hbm, raw_v, ids_sem)
    barrier = pltpu.get_barrier_semaphore()

    def peers(name, place, count, sem):
        for d in range(1, count):
            pl.semaphore_signal(
                sem, inc=1, device_id={name: lax.rem(place + d, count)}, device_id_type=MESH
            )

    inner = (("owner_1", pz, nz), ("owner_0", px, nx), ("owner_2", pc, 2))
    peers("section", section, sections, barrier)

    @pl.when(section == 0)
    def _():
        for name, place, count in inner:
            peers(name, place, count, barrier)

    w_copy.start()

    def begin(t):
        pre_copy(t).start()

        @pl.when(last)
        def _():
            cot_copy(t).start()

    each_chunk(begin)
    ids_copy.start()
    emb_copy.start()
    x_copy.start()

    @pl.when(section == 0)
    def _():
        pl.semaphore_wait(barrier, sections - 1 + sum(count - 1 for name, place, count in inner))

    @pl.when(section > 0)
    def _():
        pl.semaphore_wait(barrier, sections - 1)

    wide = GROUP * features

    def prepare():
        across = lax.broadcasted_iota(jnp.int32, (128, hidden), 1)
        flipped = lax.rem(across, features) * features + across // features

        def make_fold(b, carry):
            down = lax.broadcasted_iota(jnp.int32, (128, hidden), 0) + b * 128
            value = jnp.where(down == across, 1.0, 0.0) + jnp.where(down == flipped, 1.0, 0.0)
            part(fold, b, 128)[...] = value.astype(BF16)
            return carry

        lax.fori_loop(0, hidden // 128, make_fold, 0)
        for j in range(128 // features):
            down = lax.broadcasted_iota(jnp.int32, (128, wide), 0)
            col = lax.rem(lax.broadcasted_iota(jnp.int32, (128, wide), 1), features) + j * features
            pick[j] = jnp.where(down == col, 1.0, 0.0).astype(BF16)
        acc[...] = jnp.zeros_like(acc)
        ids_copy.wait()
        owner_lane = lax.rem(lax.broadcasted_iota(jnp.int32, (features, 4 * rows), 1) // rows, 2)
        for r in range(2):
            first, second = raw_v[r], raw_v[2 + r]
            spaced = jnp.concatenate([first, first, second, second], axis=1)
            spaced = jnp.where(owner_lane == pc, spaced, 0)
            for f in range(features):
                ids_v[f * 2 + r] = spaced[f:f + 1, :]

    near_z = nz // 2 + 1

    def gather_at(n):
        tx, tz = chip(n)
        k = n // nx
        far = k >= near_z
        home = (lax.rem(n, nx) == 0) & ((k == 0) | (k == nz - 1))
        return tx, lax.rem(tz + jnp.where(far, nz // 2, 0), nz), k, home, tx * nz + tz

    def send_ids(n, carry):
        tx, cz, k, own_chip, feature = gather_at(n)
        mine = (px * nz + k) * 2 + pc
        for r in range(2):
            there = feature * 2 + r
            home = own_chip & (pc == r)

            @pl.when(home)
            def _():
                pltpu.make_async_copy(ids_v.at[there], idr.at[mine], id_recv).start()

            @pl.when(jnp.logical_not(home))
            def _():
                remote(
                    ids_v.at[there], idr.at[mine], id_send, id_recv,
                    {"owner_0": tx, "owner_1": cz, "owner_2": r},
                ).start()
        return carry

    @pl.when(section == 0)
    def _():
        peers(*inner[0], near.at[0])

    def meet(stage):
        pl.semaphore_wait(near.at[stage], inner[stage][2] - 1)
        if stage < 2:
            peers(*inner[stage + 1], near.at[stage + 1])
        else:
            peers("section", section, sections, near.at[3])

    def exchange_ids():
        @pl.when(section > 0)
        def _():
            pl.semaphore_wait(near.at[3], 1)

        lax.fori_loop(0, nx * nz, send_ids, 0)

    w_copy.wait()

    @pl.when(jnp.logical_not(last))
    def _():
        def turn(b, carry):
            cols = pl.ds(pl.multiple_of(b * 128, 128), 128)
            wt_v[:, cols] = part(w_v, b, 128)[...].T
            return carry

        lax.fori_loop(0, hidden // 128, turn, 0)
        prepare()

    def chain_step(t):
        pre_copy(t).wait()

        @pl.when(last)
        def _():
            cot_copy(t).wait()

        @pl.when(jnp.logical_not(last))
        def _():
            down_copy(t).wait_recv()

        at = spot(t)
        incoming = rbuf[at, :]
        slope = jnp.where(pre_v[at, :] > 0, incoming, jnp.zeros_like(incoming))
        slopes[at, :] = slope

        @pl.when(last)
        def _():
            sbuf[at, :] = dot(slope, w_v[...], NT).astype(BF16)

        @pl.when(jnp.logical_not(last))
        def _():
            sbuf[at, :] = dot(slope, wt_v[...], NN).astype(BF16)

        @pl.when(section > 0)
        def _():
            down_copy(t).start()

        to, unit, place = p_place(t)

        @pl.when((section == 0) & (to > 0))
        def _():
            p_copy(t).start()

        @pl.when((section == 0) & (to == 0))
        def _():
            pbuf[place, :] = sbuf[at, :]

    block = 256

    def weight_step(m):
        size = rows * sections
        at = pl.ds(pl.multiple_of(m * size, size), size)

        def column(b, carry):
            cols = pl.ds(pl.multiple_of(b * block, block), block)
            grown = dot(x_v[at, cols], slopes[at, :], TN)
            spot = pl.ds(b * (block // 32), block // 32)
            grown = grown.reshape(block // 32, 2, 16, hidden)

            @pl.when(m == 0)
            def _():
                wacc[spot] = grown

            @pl.when(m > 0)
            def _():
                wacc[spot] = wacc[spot] + grown
            return carry

        lax.fori_loop(0, hidden // block, column, 0)

    sibling = {"owner_2": 1 - pc}
    core_copy = remote(wsend, wrecv, ac_send, ac_recv, sibling)

    def weight_core():
        def cast(k, carry):
            wsend[k] = wacc[k, 1 - pc].astype(BF16)
            return carry

        lax.fori_loop(0, nx * nz, cast, 0)
        core_copy.start()

    def x_send(d):
        to = lax.rem(px + d, nx)
        return remote(part(wx, to, nz), wxr.at[d - 1], bx_send.at[d - 1], bx_recv.at[d - 1],
                      {"owner_0": to})

    def z_send(d):
        to = lax.rem(pz + d, nz)
        return remote(wz.at[to], wzr.at[d - 1], cz_send.at[d - 1], cz_recv.at[d - 1],
                      {"owner_1": to})

    def z_first(d):
        to = lax.rem(pz + d, nz)
        return remote(part(vz, to, nx), vzr.at[d - 1], bz_send.at[d - 1], bz_recv.at[d - 1],
                      {"owner_1": to})

    def x_second(d):
        to = lax.rem(px + d, nx)
        return remote(vx.at[to], vxr.at[d - 1], cx_send.at[d - 1], cx_recv.at[d - 1],
                      {"owner_0": to})

    cut = wx.shape[-1]

    def weight_x():
        core_copy.wait_recv()

        def join(k, carry):
            both = (wacc[k, pc] + wrecv[k].astype(F32)).astype(BF16)
            wx[k] = both[:, :cut]
            vz[lax.rem(k, nz) * nx + k // nz] = both[:, cut:]
            return carry

        lax.fori_loop(0, nx * nz, join, 0)
        for d in range(1, nz):
            z_first(d).start()
        for d in range(1, nx):
            x_send(d).start()

    def weight_z():
        for d in range(1, nx):
            x_send(d).wait_recv()

        def join(k, carry):
            total = wx[px * nz + k].astype(F32)
            for d in range(nx - 1):
                total = total + wxr[d, k].astype(F32)
            wz[k] = total.astype(BF16)
            return carry

        lax.fori_loop(0, nz, join, 0)
        for d in range(1, nz):
            z_send(d).start()
        for d in range(1, nz):
            z_first(d).wait_recv()

        def join_second(k, carry):
            total = vz[pz * nx + k].astype(F32)
            for d in range(nz - 1):
                total = total + vzr[d, k].astype(F32)
            vx[k] = total.astype(BF16)
            return carry

        lax.fori_loop(0, nx, join_second, 0)
        for d in range(1, nx):
            x_second(d).start()

    def weight_end():
        total = wz[pz].astype(F32)
        for d in range(1, nz):
            z_send(d).wait_recv()
            total = total + wzr[d - 1].astype(F32)
        wg_out[:, :cut] = total * scale
        total = vx[px].astype(F32)
        for d in range(1, nx):
            x_second(d).wait_recv()
            total = total + vxr[d - 1].astype(F32)
        wg_out[:, cut:] = total * scale

    def feature_open(i):
        @pl.when(i == 0)
        def _():
            emb_copy.wait()

        @pl.when(section > 0)
        def _():
            here = part(pbuf, i, rows)
            pltpu.make_async_copy(here, here, p_recv.at[i]).wait()

        p = pbuf[pl.ds(pl.multiple_of(i * rows, rows), rows), :]
        s = dot(p, fold[...], NN).astype(BF16)
        blocks = hidden // 128
        tall = jnp.concatenate([s[:, 128 * b:128 * b + 128] for b in range(blocks)], axis=0)
        per = 128 // features
        own_row = lax.rem(lax.broadcasted_iota(jnp.int32, (rows, wide), 0), GROUP)
        own_lane = lax.broadcasted_iota(jnp.int32, (rows, wide), 1) // features
        for j in range(per):
            e = dot(tall, pick[j], NN)
            for b in range(blocks):
                kept = jnp.where(own_row == own_lane, e[rows * b:rows * b + rows], 0.0)
                spread[b * per + j] = kept.astype(BF16)

    def feature_close(i):
        for g in range(rows // GROUP):
            lhs = spread[:, GROUP * g:GROUP * g + GROUP, :].reshape(features * GROUP, wide)
            at = pl.multiple_of((i * (rows // GROUP) + g) * wide, wide)
            out = dot(lhs, emb_v[pl.ds(at, wide), :], NN)
            fg[i, :, GROUP * g:GROUP * g + GROUP, :] = out.astype(BF16).reshape(features, GROUP, lanes)

        core = lax.rem(i, 2)
        def send(step):
            tx, cz, k, own_chip, feature = gather_at(nx * nz - 1 - step)
            arrived = f_recv.at[i // 2, px, jnp.where(k >= near_z, 1, 0)]
            src = fg.at[i, feature]
            slot = pl.ds(pl.multiple_of((k * 2 + pc) * rows, rows), rows)
            dst = arr.at[i // 2, px, slot]
            home = own_chip & (pc == core)

            @pl.when(home)
            def _():
                pltpu.make_async_copy(src, dst, arrived).start()

            @pl.when(jnp.logical_not(home))
            def _():
                remote(src, dst, f_send.at[i], arrived,
                       {"owner_0": tx, "owner_1": cz, "owner_2": core}).start()

        for step in range(nx * nz):
            send(step)

    table_rows = acc.shape[1]

    def mark_rows(i):
        row = lax.broadcasted_iota(jnp.int32, (table_rows, 2 * rows), 0)

        def mark(g, carry):
            for z in range(nz):
                both = idr[(g * nz + z) * 2] + idr[(g * nz + z) * 2 + 1]
                ids = jnp.where(i < 2, both[:, :2 * rows], both[:, 2 * rows:])
                onehot[g, :, z * 2 * rows:(z + 1) * 2 * rows] = jnp.where(row == ids, 1.0, 0.0).astype(BF16)
            return carry

        lax.fori_loop(0, nx, mark, 0)

    def table_part(i, role):
        h = i // 2
        low, high = ((0, near_z), (near_z, nz))[role]
        span = pl.ds(low * 2 * rows, (high - low) * 2 * rows)

        def gather(g, carry):
            landed = arr.at[h, g, span]
            pltpu.make_async_copy(landed, landed, f_recv.at[h, g, role]).wait()
            acc[role] = acc[role] + dot(onehot[g, :, span], arr[h, g, span, :], NN)
            return carry

        lax.fori_loop(0, nx, gather, 0)

    def by_section(*values):
        chosen = values[-1]
        for n in range(sections - 1):
            chosen = jnp.where(section == n, values[n], chosen)
        return chosen

    features_at = (
        (by_section(8, 11, 17, 22), by_section(10, 13, 18, 22)),
        (by_section(12, 20, 26, 38), by_section(14, 22, 27, 38)),
        (by_section(18, 28, 33, 42), by_section(20, 30, 33, 42)),
        (by_section(26, 33, 35, 46), by_section(28, 33, 35, 46)),
    )
    mark_at = by_section(22, 34, 34, 43)
    table_at = by_section(34, 34, 34, 43)
    meet_time = by_section(5, 8, 12, 20)
    x_time = by_section(33, 33, 36, 46)
    ends = 48

    def tick(now, carry):
        for stage in range(3):
            @pl.when((section == 0) & (now == stage))
            def _():
                meet(stage)

        @pl.when(now < chunks)
        def _():
            chain_step(now)

        @pl.when(now == meet_time)
        def _():
            exchange_ids()

        @pl.when(last & (now == 6))
        def _():
            prepare()

        done = now + 1

        @pl.when((now < chunks) & (lax.rem(done, group) == 0))
        def _():
            @pl.when(done == group)
            def _():
                x_copy.wait()
            weight_step(done // group - 1)

        @pl.when(now == chunks)
        def _():
            weight_core()

        opened = micros
        closed = micros
        for n in range(micros):
            opened = jnp.where(now == features_at[n][0], n, opened)
            closed = jnp.where(now == features_at[n][1], n, closed)

        @pl.when(opened < micros)
        def _():
            feature_open(opened)

        @pl.when(closed < micros)
        def _():
            feature_close(closed)

        @pl.when(now == mark_at)
        def _():
            pltpu.make_async_copy(idr, idr, id_recv).wait()
            mark_rows(pc)

        @pl.when(now == table_at)
        def _():
            table_part(pc, 1)
            table_part(pc, 0)

        @pl.when(now == x_time)
        def _():
            weight_x()

        return carry

    lax.fori_loop(0, ends, tick, 0)

    half = table_rows // 2
    piece = half // sections

    def sib_copy(q):
        return remote(part(acc.at[q], 1 - pc, half), sib.at[q], sib_send.at[q], sib_recv.at[q], sibling)

    def y_copy(d, q):
        to = lax.rem(section + d, sections)
        return remote(part(ysend.at[q], to, piece), yrecv.at[d - 1, q],
                      y_send.at[d - 1, q], y_recv.at[d - 1, q], {"section": to})

    def settle(q):
        sib_copy(q).wait()
        mine = pl.ds(pl.multiple_of(pc * half, half), half)
        sib[q] = sib[q] + acc[q, mine, :]
        ysend[q] = sib[q].astype(BF16)
        for d in range(1, sections):
            y_copy(d, q).start()

    mark_rows(2 + pc)
    table_part(2 + pc, 1)
    sib_copy(1).start()
    table_part(2 + pc, 0)
    sib_copy(0).start()
    settle(1)
    weight_z()
    settle(0)

    def gathered(q):
        total = part(sib.at[q], section, piece)[...]
        for d in range(1, sections):
            y_copy(d, q).wait_recv()
            total = total + yrecv[d - 1, q].astype(F32)
        return total

    far_copy = remote(fsend, frecv, far_send, far_recv, {"owner_1": lax.rem(pz + nz // 2, nz)})
    fsend[...] = gathered(1).astype(BF16)
    far_copy.start()
    total = gathered(0)
    weight_end()
    far_copy.wait_recv()
    tg_out[...] = (total + frecv[...].astype(F32)) * scale

    def finish(t):
        @pl.when(section > 0)
        def _():
            down_copy(t).wait_send()

        @pl.when((section == 0) & (p_place(t)[0] > 0))
        def _():
            p_copy(t).wait_send()

    each_chunk(finish)
    some = pl.ds(0, 2 * nx * nz - 2)
    pltpu.make_async_copy(ids_v.at[some], ids_v.at[some], id_send).wait()
    for i in range(micros):
        @pl.when(pc == i % 2)
        def _():
            sent = fg.at[i, pl.ds(0, features - 2)]
            pltpu.make_async_copy(sent, sent, f_send.at[i]).wait()

        @pl.when(pc != i % 2)
        def _():
            sent = fg.at[i]
            pltpu.make_async_copy(sent, sent, f_send.at[i]).wait()
    core_copy.wait_send()
    for d in range(1, nx):
        x_send(d).wait_send()
        x_second(d).wait_send()
    for d in range(1, nz):
        z_send(d).wait_send()
        z_first(d).wait_send()
    for q in range(2):
        for d in range(1, sections):
            y_copy(d, q).wait_send()
    far_copy.wait_send()


def hand_on(a_ref, b_ref, a_out, b_out):
    a_out[...] = a_ref[...]
    b_out[...] = b_ref[...]


def per_device(weights, inputs, preact, cotangent, embeddings, row_ids):
    sections = lax.axis_size("section")
    nx, nz, cores = (lax.axis_size(a) for a in OWNER)
    micros, batch_rows, hidden = cotangent.shape
    quarter, features, width = embeddings.shape[1:]
    total = micros * batch_rows
    owners = nx * nz * cores
    scale = 1.0 / math.sqrt(total * owners)
    table_rows = 1024
    ids_shape = (owners, 1, 2 * cores * quarter)
    dma = pltpu.SemaphoreType.DMA
    vmem = pl.BlockSpec(memory_space=pltpu.VMEM)
    hbm = pl.BlockSpec(memory_space=pl.ANY)
    chunks = 2 * sections * micros
    rows = total // (micros * sections)
    wide = GROUP * features
    part = hidden // owners
    half = table_rows // 2
    cut = hidden * 3 // 4
    V = pltpu.VMEM
    weight_grad, table_grad = pl.pallas_call(
        functools.partial(step_kernel, (micros, sections, nx, nz, features), scale),
        out_shape=(V((part, hidden), F32), V((half // sections, width), F32)),
        in_specs=[hbm] * 6,
        out_specs=(vmem, vmem),
        scratch_shapes=[
            V((hidden, hidden), BF16),
            V((hidden, hidden), BF16),
            V((total, hidden), BF16),
            V((total, hidden), BF16),
            V((micros * quarter * features, width), BF16),
            V((micros, features, quarter), jnp.int32),
            V(ids_shape, jnp.int32),
            V((total, hidden), BF16),
            V((total, hidden), BF16),
            V((total, hidden), BF16),
            V((micros * quarter, hidden), BF16),
            V((nx * nz, 2, part, hidden), F32),
            V((nx * nz, part, hidden), BF16),
            V((nx * nz, part, hidden), BF16),
            V((nx * nz, part, cut), BF16),
            V((nx - 1, nz, part, cut), BF16),
            V((nz, part, cut), BF16),
            V((nz - 1, part, cut), BF16),
            V((nx * nz, part, hidden - cut), BF16),
            V((nz - 1, nx, part, hidden - cut), BF16),
            V((nx, part, hidden - cut), BF16),
            V((nx - 1, part, hidden - cut), BF16),
            V((hidden, hidden), BF16),
            V((128 // features, 128, wide), BF16),
            V((features, rows, wide), BF16),
            V((micros, features, rows, width), BF16),
            V((micros // 2, nx, nz * 2 * rows, width), BF16),
            V(ids_shape, jnp.int32),
            V((nx, table_rows, nz * 2 * rows), BF16),
            V((2, table_rows, width), F32),
            V((2, half, width), F32),
            V((2, half, width), BF16),
            V((sections - 1, 2, half // sections, width), BF16),
            V((half // sections, width), BF16),
            V((half // sections, width), BF16),
            pltpu.SemaphoreType.REGULAR((4,)),
            dma, dma, dma((chunks,)), dma, dma, dma((chunks,)), dma((chunks,)),
            dma((micros,)), dma((chunks,)),
            dma, dma, dma((micros,)), dma((micros // 2, nx, 2)),
            dma, dma, dma((nx - 1,)), dma((nx - 1,)), dma((nz - 1,)), dma((nz - 1,)),
            dma((nz - 1,)), dma((nz - 1,)), dma((nx - 1,)), dma((nx - 1,)),
            dma((2,)), dma((2,)), dma((sections - 1, 2)), dma((sections - 1, 2)), dma, dma,
        ],
        compiler_params=pltpu.CompilerParams(
            collective_id=0, has_side_effects=True, vmem_limit_bytes=60 * 1024 * 1024
        ),
    )(
        weights[0],
        inputs.reshape(total, hidden),
        preact.reshape(total, hidden),
        cotangent.reshape(total, hidden),
        embeddings.reshape(micros * quarter * features, width),
        row_ids.transpose(0, 2, 1),
    )
    weight_grad, table_grad = pl.pallas_call(
        hand_on,
        out_shape=(
            jax.ShapeDtypeStruct(weight_grad.shape, F32),
            jax.ShapeDtypeStruct(table_grad.shape, F32),
        ),
        in_specs=[vmem] * 2,
        out_specs=(vmem, vmem),
    )(pltpu.with_memory_space_constraint(weight_grad, pltpu.VMEM), pltpu.with_memory_space_constraint(table_grad, pltpu.VMEM))
    return (weight_grad[None], table_grad[None])


def solution(mesh):
    finer = Mesh(
        mesh.devices.reshape(mesh.shape["section"], 4, 8, 2),
        ("section", "owner_0", "owner_1", "owner_2"),
    )
    placed = (
        P("section", None, None),
        P("section", None, OWNER, None),
        P("section", None, OWNER, None),
        P(None, OWNER, None),
        P(None, OWNER_SECTION, None, None),
        P(None, OWNER_SECTION, None),
    )
    return jax.shard_map(
        per_device,
        mesh=finer,
        in_specs=placed,
        out_specs=(P("section", OWNER, None), P(OWNER, "section", None)),
        check_vma=False,
    )
```

```python
import functools
import math

import jax
import jax.numpy as jnp
from jax import lax
from jax.experimental import pallas as pl
from jax.experimental.pallas import tpu as pltpu
from jax.sharding import Mesh
from jax.sharding import PartitionSpec as P

OWNER = ("owner_0", "owner_1", "owner_2")
OWNER_SECTION = ("owner_0", "owner_1", "owner_2", "section")
MESH = pl.DeviceIdType.MESH
BF16 = jnp.bfloat16
F32 = jnp.float32
NN = (((1,), (0,)), ((), ()))
NT = (((1,), (1,)), ((), ()))
TN = (((0,), (0,)), ((), ()))
GROUP = 16


def dot(a, b, dims):
    return lax.dot_general(a, b, dims, preferred_element_type=F32)


def step_kernel(
    dims, scale,
    w_hbm, x_hbm, pre_hbm, cot_hbm, emb_hbm, ids_hbm,
    wg_out, tg_out,
    w_v, wt_v, x_v, pre_v, emb_v, raw_v, ids_v, rbuf, sbuf, slopes, pbuf, wacc, wsend, wrecv, wx, wxr, wz, wzr, vz, vzr, vx, vxr,
    fold, pick, spread, fg, arr, idr, onehot, acc, sib, ysend, yrecv, fsend, frecv,
    near, w_sem, x_sem, pre_sem, emb_sem, ids_sem, in_sem, out_sem, p_recv, p_send,
    id_send, id_recv, f_send, f_recv, ac_send, ac_recv, bx_send, bx_recv, cz_send, cz_recv, bz_send, bz_recv, cx_send, cx_recv,
    sib_send, sib_recv, y_send, y_recv, far_send, far_recv,
):
    micros, sections, nx, nz, features = dims
    section = lax.axis_index("section")
    px = lax.axis_index("owner_0")
    pz = lax.axis_index("owner_1")
    pc = lax.axis_index("owner_2")
    rows = pre_v.shape[0] // (micros * sections)
    fine = rows // 2
    group = 2 * sections
    chunks = group * micros
    hidden = w_v.shape[0]
    lanes = emb_v.shape[1]
    last = section == sections - 1

    def part(ref, t, size):
        return ref.at[pl.ds(pl.multiple_of(t * size, size), size)]

    def spot(t):
        return pl.ds(pl.multiple_of(t * fine, fine), fine)

    def each_chunk(body):
        def one(t, carry):
            body(t)
            return carry

        lax.fori_loop(0, chunks, one, 0)

    def pre_copy(t):
        return pltpu.make_async_copy(pre_hbm.at[spot(t)], pre_v.at[spot(t)], pre_sem.at[t])

    def cot_copy(t):
        return pltpu.make_async_copy(cot_hbm.at[spot(t)], rbuf.at[spot(t)], in_sem.at[t])

    def remote(src, dst, send, recv, where):
        return pltpu.make_async_remote_copy(
            src_ref=src, dst_ref=dst, send_sem=send, recv_sem=recv,
            device_id=where, device_id_type=MESH,
        )

    def down_copy(t):
        return remote(
            sbuf.at[spot(t)], rbuf.at[spot(t)], out_sem.at[t], in_sem.at[t],
            {"section": lax.rem(section + sections - 1, sections)},
        )

    def p_place(t):
        unit = t // group
        start = unit * rows + lax.rem(t, 2) * fine
        return lax.rem(t, group) // 2, unit, pl.ds(pl.multiple_of(start, fine), fine)

    def p_copy(t):
        to, unit, at = p_place(t)
        return remote(
            sbuf.at[spot(t)], pbuf.at[at], p_send.at[t], p_recv.at[unit], {"section": to}
        )

    def chip(n):
        dx = lax.rem(n, nx)
        k = n // nx
        dz = ((k + 1) // 2) * (2 * lax.rem(k, 2) - 1)
        return lax.rem(px + dx, nx), lax.rem(pz + dz + nz, nz)

    w_copy = pltpu.make_async_copy(w_hbm, w_v, w_sem)
    x_copy = pltpu.make_async_copy(x_hbm, x_v, x_sem)
    emb_copy = pltpu.make_async_copy(emb_hbm, emb_v, emb_sem)
    ids_copy = pltpu.make_async_copy(ids_hbm, raw_v, ids_sem)
    barrier = pltpu.get_barrier_semaphore()

    def peers(name, place, count, sem):
        for d in range(1, count):
            pl.semaphore_signal(
                sem, inc=1, device_id={name: lax.rem(place + d, count)}, device_id_type=MESH
            )

    inner = (("owner_1", pz, nz), ("owner_0", px, nx), ("owner_2", pc, 2))
    peers("section", section, sections, barrier)

    @pl.when(section == 0)
    def _():
        for name, place, count in inner:
            peers(name, place, count, barrier)

    w_copy.start()

    def begin(t):
        pre_copy(t).start()

        @pl.when(last)
        def _():
            cot_copy(t).start()

    each_chunk(begin)
    ids_copy.start()
    emb_copy.start()
    x_copy.start()

    @pl.when(section == 0)
    def _():
        pl.semaphore_wait(barrier, sections - 1 + sum(count - 1 for name, place, count in inner))

    @pl.when(section > 0)
    def _():
        pl.semaphore_wait(barrier, sections - 1)

    wide = GROUP * features

    def prepare():
        across = lax.broadcasted_iota(jnp.int32, (128, hidden), 1)
        flipped = lax.rem(across, features) * features + across // features

        def make_fold(b, carry):
            down = lax.broadcasted_iota(jnp.int32, (128, hidden), 0) + b * 128
            value = jnp.where(down == across, 1.0, 0.0) + jnp.where(down == flipped, 1.0, 0.0)
            part(fold, b, 128)[...] = value.astype(BF16)
            return carry

        lax.fori_loop(0, hidden // 128, make_fold, 0)
        for j in range(128 // features):
            down = lax.broadcasted_iota(jnp.int32, (128, wide), 0)
            col = lax.rem(lax.broadcasted_iota(jnp.int32, (128, wide), 1), features) + j * features
            pick[j] = jnp.where(down == col, 1.0, 0.0).astype(BF16)
        acc[...] = jnp.zeros_like(acc)
        ids_copy.wait()
        owner_lane = lax.rem(lax.broadcasted_iota(jnp.int32, (features, 4 * rows), 1) // rows, 2)
        for r in range(2):
            first, second = raw_v[r], raw_v[2 + r]
            spaced = jnp.concatenate([first, first, second, second], axis=1)
            spaced = jnp.where(owner_lane == pc, spaced, 0)
            for f in range(features):
                ids_v[f * 2 + r] = spaced[f:f + 1, :]

    near_z = nz // 2 + 1

    def gather_at(n):
        tx, tz = chip(n)
        k = n // nx
        far = k >= near_z
        home = (lax.rem(n, nx) == 0) & ((k == 0) | (k == nz - 1))
        return tx, lax.rem(tz + jnp.where(far, nz // 2, 0), nz), k, home, tx * nz + tz

    def send_ids(n, carry):
        tx, cz, k, own_chip, feature = gather_at(n)
        mine = (px * nz + k) * 2 + pc
        for r in range(2):
            there = feature * 2 + r
            home = own_chip & (pc == r)

            @pl.when(home)
            def _():
                pltpu.make_async_copy(ids_v.at[there], idr.at[mine], id_recv).start()

            @pl.when(jnp.logical_not(home))
            def _():
                remote(
                    ids_v.at[there], idr.at[mine], id_send, id_recv,
                    {"owner_0": tx, "owner_1": cz, "owner_2": r},
                ).start()
        return carry

    @pl.when(section == 0)
    def _():
        peers(*inner[0], near.at[0])

    def meet(stage):
        pl.semaphore_wait(near.at[stage], inner[stage][2] - 1)
        if stage < 2:
            peers(*inner[stage + 1], near.at[stage + 1])
        else:
            peers("section", section, sections, near.at[3])

    def exchange_ids():
        @pl.when(section > 0)
        def _():
            pl.semaphore_wait(near.at[3], 1)

        lax.fori_loop(0, nx * nz, send_ids, 0)

    w_copy.wait()

    @pl.when(jnp.logical_not(last))
    def _():
        def turn(b, carry):
            cols = pl.ds(pl.multiple_of(b * 128, 128), 128)
            wt_v[:, cols] = part(w_v, b, 128)[...].T
            return carry

        lax.fori_loop(0, hidden // 128, turn, 0)
        prepare()

    def chain_step(t):
        pre_copy(t).wait()

        @pl.when(last)
        def _():
            cot_copy(t).wait()

        @pl.when(jnp.logical_not(last))
        def _():
            down_copy(t).wait_recv()

        at = spot(t)
        incoming = rbuf[at, :]
        slope = jnp.where(pre_v[at, :] > 0, incoming, jnp.zeros_like(incoming))
        slopes[at, :] = slope

        @pl.when(last)
        def _():
            sbuf[at, :] = dot(slope, w_v[...], NT).astype(BF16)

        @pl.when(jnp.logical_not(last))
        def _():
            sbuf[at, :] = dot(slope, wt_v[...], NN).astype(BF16)

        @pl.when(section > 0)
        def _():
            down_copy(t).start()

        to, unit, place = p_place(t)

        @pl.when((section == 0) & (to > 0))
        def _():
            p_copy(t).start()

        @pl.when((section == 0) & (to == 0))
        def _():
            pbuf[place, :] = sbuf[at, :]

    block = 256

    def weight_step(m):
        size = rows * sections
        at = pl.ds(pl.multiple_of(m * size, size), size)

        def column(b, carry):
            cols = pl.ds(pl.multiple_of(b * block, block), block)
            grown = dot(x_v[at, cols], slopes[at, :], TN)
            spot = pl.ds(b * (block // 32), block // 32)
            grown = grown.reshape(block // 32, 2, 16, hidden)

            @pl.when(m == 0)
            def _():
                wacc[spot] = grown

            @pl.when(m > 0)
            def _():
                wacc[spot] = wacc[spot] + grown
            return carry

        lax.fori_loop(0, hidden // block, column, 0)

    sibling = {"owner_2": 1 - pc}
    core_copy = remote(wsend, wrecv, ac_send, ac_recv, sibling)

    def weight_core():
        def cast(k, carry):
            wsend[k] = wacc[k, 1 - pc].astype(BF16)
            return carry

        lax.fori_loop(0, nx * nz, cast, 0)
        core_copy.start()

    def x_send(d):
        to = lax.rem(px + d, nx)
        return remote(part(wx, to, nz), wxr.at[d - 1], bx_send.at[d - 1], bx_recv.at[d - 1],
                      {"owner_0": to})

    def z_send(d):
        to = lax.rem(pz + d, nz)
        return remote(wz.at[to], wzr.at[d - 1], cz_send.at[d - 1], cz_recv.at[d - 1],
                      {"owner_1": to})

    def z_first(d):
        to = lax.rem(pz + d, nz)
        return remote(part(vz, to, nx), vzr.at[d - 1], bz_send.at[d - 1], bz_recv.at[d - 1],
                      {"owner_1": to})

    def x_second(d):
        to = lax.rem(px + d, nx)
        return remote(vx.at[to], vxr.at[d - 1], cx_send.at[d - 1], cx_recv.at[d - 1],
                      {"owner_0": to})

    cut = wx.shape[-1]

    def weight_x():
        core_copy.wait_recv()

        def join(k, carry):
            both = (wacc[k, pc] + wrecv[k].astype(F32)).astype(BF16)
            wx[k] = both[:, :cut]
            vz[lax.rem(k, nz) * nx + k // nz] = both[:, cut:]
            return carry

        lax.fori_loop(0, nx * nz, join, 0)
        for d in range(1, nz):
            z_first(d).start()
        for d in range(1, nx):
            x_send(d).start()

    def weight_z():
        for d in range(1, nx):
            x_send(d).wait_recv()

        def join(k, carry):
            total = wx[px * nz + k].astype(F32)
            for d in range(nx - 1):
                total = total + wxr[d, k].astype(F32)
            wz[k] = total.astype(BF16)
            return carry

        lax.fori_loop(0, nz, join, 0)
        for d in range(1, nz):
            z_send(d).start()
        for d in range(1, nz):
            z_first(d).wait_recv()

        def join_second(k, carry):
            total = vz[pz * nx + k].astype(F32)
            for d in range(nz - 1):
                total = total + vzr[d, k].astype(F32)
            vx[k] = total.astype(BF16)
            return carry

        lax.fori_loop(0, nx, join_second, 0)
        for d in range(1, nx):
            x_second(d).start()

    def weight_end():
        total = wz[pz].astype(F32)
        for d in range(1, nz):
            z_send(d).wait_recv()
            total = total + wzr[d - 1].astype(F32)
        wg_out[:, :cut] = total * scale
        total = vx[px].astype(F32)
        for d in range(1, nx):
            x_second(d).wait_recv()
            total = total + vxr[d - 1].astype(F32)
        wg_out[:, cut:] = total * scale

    def feature_open(i):
        @pl.when(i == 0)
        def _():
            emb_copy.wait()

        @pl.when(section > 0)
        def _():
            here = part(pbuf, i, rows)
            pltpu.make_async_copy(here, here, p_recv.at[i]).wait()

        p = pbuf[pl.ds(pl.multiple_of(i * rows, rows), rows), :]
        s = dot(p, fold[...], NN).astype(BF16)
        blocks = hidden // 128
        tall = jnp.concatenate([s[:, 128 * b:128 * b + 128] for b in range(blocks)], axis=0)
        per = 128 // features
        own_row = lax.rem(lax.broadcasted_iota(jnp.int32, (rows, wide), 0), GROUP)
        own_lane = lax.broadcasted_iota(jnp.int32, (rows, wide), 1) // features
        for j in range(per):
            e = dot(tall, pick[j], NN)
            for b in range(blocks):
                kept = jnp.where(own_row == own_lane, e[rows * b:rows * b + rows], 0.0)
                spread[b * per + j] = kept.astype(BF16)

    def feature_close(i):
        for g in range(rows // GROUP):
            lhs = spread[:, GROUP * g:GROUP * g + GROUP, :].reshape(features * GROUP, wide)
            at = pl.multiple_of((i * (rows // GROUP) + g) * wide, wide)
            out = dot(lhs, emb_v[pl.ds(at, wide), :], NN)
            fg[i, :, GROUP * g:GROUP * g + GROUP, :] = out.astype(BF16).reshape(features, GROUP, lanes)

        core = lax.rem(i, 2)
        def send(step):
            tx, cz, k, own_chip, feature = gather_at(nx * nz - 1 - step)
            arrived = f_recv.at[i // 2, px, jnp.where(k >= near_z, 1, 0)]
            src = fg.at[i, feature]
            slot = pl.ds(pl.multiple_of((k * 2 + pc) * rows, rows), rows)
            dst = arr.at[i // 2, px, slot]
            home = own_chip & (pc == core)

            @pl.when(home)
            def _():
                pltpu.make_async_copy(src, dst, arrived).start()

            @pl.when(jnp.logical_not(home))
            def _():
                remote(src, dst, f_send.at[i], arrived,
                       {"owner_0": tx, "owner_1": cz, "owner_2": core}).start()

        for step in range(nx * nz):
            send(step)

    table_rows = acc.shape[1]

    def mark_rows(i):
        row = lax.broadcasted_iota(jnp.int32, (table_rows, 2 * rows), 0)

        def mark(g, carry):
            for z in range(nz):
                both = idr[(g * nz + z) * 2] + idr[(g * nz + z) * 2 + 1]
                ids = jnp.where(i < 2, both[:, :2 * rows], both[:, 2 * rows:])
                onehot[g, :, z * 2 * rows:(z + 1) * 2 * rows] = jnp.where(row == ids, 1.0, 0.0).astype(BF16)
            return carry

        lax.fori_loop(0, nx, mark, 0)

    def table_part(i, role):
        h = i // 2
        low, high = ((0, near_z), (near_z, nz))[role]
        span = pl.ds(low * 2 * rows, (high - low) * 2 * rows)

        def gather(g, carry):
            landed = arr.at[h, g, span]
            pltpu.make_async_copy(landed, landed, f_recv.at[h, g, role]).wait()
            acc[role] = acc[role] + dot(onehot[g, :, span], arr[h, g, span, :], NN)
            return carry

        lax.fori_loop(0, nx, gather, 0)

    def by_section(*values):
        chosen = values[-1]
        for n in range(sections - 1):
            chosen = jnp.where(section == n, values[n], chosen)
        return chosen

    features_at = (
        (by_section(8, 11, 17, 22), by_section(10, 13, 18, 22)),
        (by_section(12, 20, 26, 38), by_section(14, 22, 27, 38)),
        (by_section(18, 28, 33, 42), by_section(20, 30, 33, 42)),
        (by_section(26, 33, 35, 46), by_section(28, 33, 35, 46)),
    )
    mark_at = by_section(22, 34, 34, 43)
    table_at = by_section(34, 34, 34, 43)
    meet_time = by_section(5, 8, 12, 20)
    x_time = by_section(33, 33, 36, 46)
    ends = 48

    def tick(now, carry):
        for stage in range(3):
            @pl.when((section == 0) & (now == stage))
            def _():
                meet(stage)

        @pl.when(now < chunks)
        def _():
            chain_step(now)

        @pl.when(now == meet_time)
        def _():
            exchange_ids()

        @pl.when(last & (now == 6))
        def _():
            prepare()

        done = now + 1

        @pl.when((now < chunks) & (lax.rem(done, group) == 0))
        def _():
            @pl.when(done == group)
            def _():
                x_copy.wait()
            weight_step(done // group - 1)

        @pl.when(now == chunks)
        def _():
            weight_core()

        opened = micros
        closed = micros
        for n in range(micros):
            opened = jnp.where(now == features_at[n][0], n, opened)
            closed = jnp.where(now == features_at[n][1], n, closed)

        @pl.when(opened < micros)
        def _():
            feature_open(opened)

        @pl.when(closed < micros)
        def _():
            feature_close(closed)

        @pl.when(now == mark_at)
        def _():
            pltpu.make_async_copy(idr, idr, id_recv).wait()
            mark_rows(pc)

        @pl.when(now == table_at)
        def _():
            table_part(pc, 1)
            table_part(pc, 0)

        @pl.when(now == x_time)
        def _():
            weight_x()

        return carry

    lax.fori_loop(0, ends, tick, 0)

    half = table_rows // 2
    piece = half // sections

    def sib_copy(q):
        return remote(part(acc.at[q], 1 - pc, half), sib.at[q], sib_send.at[q], sib_recv.at[q], sibling)

    def y_copy(d, q):
        to = lax.rem(section + d, sections)
        return remote(part(ysend.at[q], to, piece), yrecv.at[d - 1, q],
                      y_send.at[d - 1, q], y_recv.at[d - 1, q], {"section": to})

    def settle(q):
        sib_copy(q).wait()
        mine = pl.ds(pl.multiple_of(pc * half, half), half)
        sib[q] = sib[q] + acc[q, mine, :]
        ysend[q] = sib[q].astype(BF16)
        for d in range(1, sections):
            y_copy(d, q).start()

    mark_rows(2 + pc)
    table_part(2 + pc, 1)
    sib_copy(1).start()
    table_part(2 + pc, 0)
    sib_copy(0).start()
    settle(1)
    weight_z()
    settle(0)

    def gathered(q):
        total = part(sib.at[q], section, piece)[...]
        for d in range(1, sections):
            y_copy(d, q).wait_recv()
            total = total + yrecv[d - 1, q].astype(F32)
        return total

    far_copy = remote(fsend, frecv, far_send, far_recv, {"owner_1": lax.rem(pz + nz // 2, nz)})
    fsend[...] = gathered(1).astype(BF16)
    far_copy.start()
    total = gathered(0)
    weight_end()
    far_copy.wait_recv()
    tg_out[...] = (total + frecv[...].astype(F32)) * scale

    def finish(t):
        @pl.when(section > 0)
        def _():
            down_copy(t).wait_send()

        @pl.when((section == 0) & (p_place(t)[0] > 0))
        def _():
            p_copy(t).wait_send()

    each_chunk(finish)
    some = pl.ds(0, 2 * nx * nz - 2)
    pltpu.make_async_copy(ids_v.at[some], ids_v.at[some], id_send).wait()
    for i in range(micros):
        @pl.when(pc == i % 2)
        def _():
            sent = fg.at[i, pl.ds(0, features - 2)]
            pltpu.make_async_copy(sent, sent, f_send.at[i]).wait()

        @pl.when(pc != i % 2)
        def _():
            sent = fg.at[i]
            pltpu.make_async_copy(sent, sent, f_send.at[i]).wait()
    core_copy.wait_send()
    for d in range(1, nx):
        x_send(d).wait_send()
        x_second(d).wait_send()
    for d in range(1, nz):
        z_send(d).wait_send()
        z_first(d).wait_send()
    for q in range(2):
        for d in range(1, sections):
            y_copy(d, q).wait_send()
    far_copy.wait_send()


def hand_on(a_ref, b_ref, a_out, b_out):
    a_out[...] = a_ref[...]
    b_out[...] = b_ref[...]


def per_device(weights, inputs, preact, cotangent, embeddings, row_ids):
    sections = lax.axis_size("section")
    nx, nz, cores = (lax.axis_size(a) for a in OWNER)
    micros, batch_rows, hidden = cotangent.shape
    quarter, features, width = embeddings.shape[1:]
    total = micros * batch_rows
    owners = nx * nz * cores
    scale = 1.0 / math.sqrt(total * owners)
    table_rows = 1024
    ids_shape = (owners, 1, 2 * cores * quarter)
    dma = pltpu.SemaphoreType.DMA
    vmem = pl.BlockSpec(memory_space=pltpu.VMEM)
    hbm = pl.BlockSpec(memory_space=pl.ANY)
    chunks = 2 * sections * micros
    rows = total // (micros * sections)
    wide = GROUP * features
    part = hidden // owners
    half = table_rows // 2
    cut = hidden * 5 // 8
    V = pltpu.VMEM
    weight_grad, table_grad = pl.pallas_call(
        functools.partial(step_kernel, (micros, sections, nx, nz, features), scale),
        out_shape=(V((part, hidden), F32), V((half // sections, width), F32)),
        in_specs=[hbm] * 6,
        out_specs=(vmem, vmem),
        scratch_shapes=[
            V((hidden, hidden), BF16),
            V((hidden, hidden), BF16),
            V((total, hidden), BF16),
            V((total, hidden), BF16),
            V((micros * quarter * features, width), BF16),
            V((micros, features, quarter), jnp.int32),
            V(ids_shape, jnp.int32),
            V((total, hidden), BF16),
            V((total, hidden), BF16),
            V((total, hidden), BF16),
            V((micros * quarter, hidden), BF16),
            V((nx * nz, 2, part, hidden), F32),
            V((nx * nz, part, hidden), BF16),
            V((nx * nz, part, hidden), BF16),
            V((nx * nz, part, cut), BF16),
            V((nx - 1, nz, part, cut), BF16),
            V((nz, part, cut), BF16),
            V((nz - 1, part, cut), BF16),
            V((nx * nz, part, hidden - cut), BF16),
            V((nz - 1, nx, part, hidden - cut), BF16),
            V((nx, part, hidden - cut), BF16),
            V((nx - 1, part, hidden - cut), BF16),
            V((hidden, hidden), BF16),
            V((128 // features, 128, wide), BF16),
            V((features, rows, wide), BF16),
            V((micros, features, rows, width), BF16),
            V((micros // 2, nx, nz * 2 * rows, width), BF16),
            V(ids_shape, jnp.int32),
            V((nx, table_rows, nz * 2 * rows), BF16),
            V((2, table_rows, width), F32),
            V((2, half, width), F32),
            V((2, half, width), BF16),
            V((sections - 1, 2, half // sections, width), BF16),
            V((half // sections, width), BF16),
            V((half // sections, width), BF16),
            pltpu.SemaphoreType.REGULAR((4,)),
            dma, dma, dma((chunks,)), dma, dma, dma((chunks,)), dma((chunks,)),
            dma((micros,)), dma((chunks,)),
            dma, dma, dma((micros,)), dma((micros // 2, nx, 2)),
            dma, dma, dma((nx - 1,)), dma((nx - 1,)), dma((nz - 1,)), dma((nz - 1,)),
            dma((nz - 1,)), dma((nz - 1,)), dma((nx - 1,)), dma((nx - 1,)),
            dma((2,)), dma((2,)), dma((sections - 1, 2)), dma((sections - 1, 2)), dma, dma,
        ],
        compiler_params=pltpu.CompilerParams(
            collective_id=0, has_side_effects=True, vmem_limit_bytes=60 * 1024 * 1024
        ),
    )(
        weights[0],
        inputs.reshape(total, hidden),
        preact.reshape(total, hidden),
        cotangent.reshape(total, hidden),
        embeddings.reshape(micros * quarter * features, width),
        row_ids.transpose(0, 2, 1),
    )
    weight_grad, table_grad = pl.pallas_call(
        hand_on,
        out_shape=(
            jax.ShapeDtypeStruct(weight_grad.shape, F32),
            jax.ShapeDtypeStruct(table_grad.shape, F32),
        ),
        in_specs=[vmem] * 2,
        out_specs=(vmem, vmem),
    )(pltpu.with_memory_space_constraint(weight_grad, pltpu.VMEM), pltpu.with_memory_space_constraint(table_grad, pltpu.VMEM))
    return (weight_grad[None], table_grad[None])


def solution(mesh):
    finer = Mesh(
        mesh.devices.reshape(mesh.shape["section"], 4, 8, 2),
        ("section", "owner_0", "owner_1", "owner_2"),
    )
    placed = (
        P("section", None, None),
        P("section", None, OWNER, None),
        P("section", None, OWNER, None),
        P(None, OWNER, None),
        P(None, OWNER_SECTION, None, None),
        P(None, OWNER_SECTION, None),
    )
    return jax.shard_map(
        per_device,
        mesh=finer,
        in_specs=placed,
        out_specs=(P("section", OWNER, None), P(OWNER, "section", None)),
        check_vma=False,
    )
```
